32 devices in a mesh: layer: 2 (over x), row: 4 (over z), col: 4 (over y, core).
Axes of the slice: x: 2, y: 2, z: 4, core: 2. Of those that a mesh axis runs over, the one named last changes fastest.
Arguments:
- left_matrix: float32 [2, 1024, 16384], P(None, 'row', 'col'), may hold values from -6 to 6
- right_matrix: float32 [2, 16384, 512], P(None, 'row', 'col'), may hold values from -0.03125 to 0.03125
Outputs:
- product: float32 [2, 1024, 512], P(None, 'row', 'col')
The draws below stay inside these ranges and needn't reach their ends.
All inputs are finite; a program needn't handle non-finite values.
Results may differ from the reference program's by a relative error of at most 0.000071.
Values sent between devices are 32-bit elements; how exact they have to be, the bound alone decides.
A program may use at most 128 MiB of HBM per device.

```python
import jax
import jax.numpy as jnp
from jax import lax

K = 16384
M = 1024
NC = 512


def block_scale(key, dims, cuts, smallest, largest):
    gain, own = 1.0, jax.random.fold_in(key, 6)
    for axis_at, shards_of in cuts:
        draws = jnp.exp(jax.random.uniform(jax.random.fold_in(own, axis_at), (shards_of,), jnp.float32, smallest / len(cuts), largest / len(cuts)))
        gain = gain * jnp.repeat(draws, dims[axis_at] // shards_of).reshape([-1 if axis == axis_at else 1 for axis in range(len(dims))])
    return gain


def gaussian(own_key, dims, width, most, cuts=(), kind=jnp.bfloat16):
    entries = width * jax.random.normal(own_key, dims, jnp.float32)
    if cuts:
        entries = entries * block_scale(own_key, dims, cuts, -0.22, 0.18)
    return jnp.clip(entries, -most, most).astype(kind)


def setup_inputs(seed: int = 0) -> dict:
    splits = jax.random.split(jax.random.key(seed), 3)
    left_matrix = gaussian(splits[0], (2, M, K), 1.0, 6.0, ((1, 4), (2, 4)), jnp.float32)
    right_matrix = gaussian(splits[1], (2, K, NC), (2 * K) ** -0.5, 0.03125, ((1, 4), (2, 4)), jnp.float32)
    return dict(left_matrix=left_matrix, right_matrix=right_matrix)


def reference(left_matrix, right_matrix):
    highest = lax.Precision.HIGHEST
    left_real = left_matrix[0]
    left_imag = left_matrix[1]
    right_real = right_matrix[0]
    right_imag = right_matrix[1]
    first_term = jnp.dot(left_real, right_real, precision=highest, preferred_element_type=jnp.float32)
    second_term = jnp.dot(left_imag, right_imag, precision=highest, preferred_element_type=jnp.float32)
    third_term = jnp.dot(left_real + left_imag, right_real + right_imag, precision=highest, preferred_element_type=jnp.float32)
    return jnp.stack([first_term - second_term, third_term - first_term - second_term])
```

```python
import functools

import jax
import jax.numpy as jnp
from jax import lax
from jax.experimental import pallas as pl
from jax.experimental.pallas import tpu as pltpu
from jax.sharding import PartitionSpec as P

CHUNKS = 16
FINE = 2
GROUPS = 4
MESH = pl.DeviceIdType.MESH


def kernel(rows, left, right, out, abuf, bbuf, xbuf, ebuf, acc, xacc, xout, xin, pout, pin, qout, qin,
           own_sem, bsend, rsend, brecv, bown, ysend, yrecv, xsend, xrecv, esem, csend, crecv,
           psend, precv, qsend, qrecv, turn):
    x = lax.axis_index("layer")
    z = lax.axis_index("row")
    col = lax.axis_index("col")
    y = col // 2
    c = col % 2
    height = left.shape[1]
    width = right.shape[2]
    share = abuf.shape[3]
    step = share // CHUNKS
    fine = step // FINE
    tall = height // GROUPS
    wide = share // GROUPS
    last = rows - 1
    tail = CHUNKS - 1
    base = x * share
    parity = z % 2
    at_low, at_high = z == 0, z == last
    at_end = at_low | at_high
    lends = (at_low & (c == 1)) | (at_high & (c == 0))
    helps = ((z == 1) & (c == 1)) | ((z == last - 1) & (c == 0))
    inward = jnp.where(at_low, 1, last - 1)
    outward = jnp.where(z == 1, 0, last)
    far = jnp.where(z < rows // 2, last, 0)
    lent_slot = jnp.where(at_low, 0, (last - 1) // 2)
    lends_own = lends & (y == lent_slot)
    lends_relayed = lends & (y != lent_slot)

    def other(**where):
        return dict(device_id=where, device_id_type=MESH)

    partner = dict(col=y * 2 + 1 - c)
    across = dict(col=(1 - y) * 2 + c)
    copy_x = dict(layer=1 - x)

    barrier = pltpu.get_barrier_semaphore()
    for where in (partner, across, copy_x):
        pl.semaphore_signal(barrier, inc=1, **other(**where))

    @pl.when(z > 0)
    def _():
        for core in range(2):
            pl.semaphore_signal(barrier, inc=1, **other(row=z - 1, col=y * 2 + core))

    @pl.when(z < last)
    def _():
        for core in range(2):
            pl.semaphore_signal(barrier, inc=1, **other(row=z + 1, col=y * 2 + core))

    own_copy = pltpu.make_async_copy(left.at[:, :, pl.ds(base, share)], abuf.at[y], own_sem)
    own_copy.start()
    acc[...] = jnp.zeros_like(acc)
    xacc[...] = jnp.zeros_like(xacc)
    pl.semaphore_wait(barrier, 3 + 2 * ((z > 0).astype(jnp.int32) + (z < last).astype(jnp.int32)))

    def span(i):
        return pl.ds(pl.multiple_of(i * step, step), step)

    def source_span(i):
        return pl.ds(pl.multiple_of(base + i * step, step), step)

    def fine_span(u):
        return pl.ds(pl.multiple_of(u * fine, fine), fine)

    def fine_source(u):
        return pl.ds(pl.multiple_of(base + u * fine, fine), fine)

    def half(h):
        return pl.ds(pl.multiple_of(h * width, width), width)

    def group(g):
        return pl.ds(pl.multiple_of(g * tall, tall), tall)

    def piece_rows(i):
        return group(i // GROUPS)

    def piece_cols(i):
        return pl.ds(pl.multiple_of((i % GROUPS) * wide, wide), wide)

    def piece_source(i):
        return pl.ds(pl.multiple_of(base + (i % GROUPS) * wide, step), wide)

    whole_source = pl.ds(pl.multiple_of(base, step), share)

    def b_copy(u, way, row):
        return pltpu.make_async_remote_copy(
            src_ref=right.at[:, fine_source(u), :],
            dst_ref=bbuf.at[z // 2, c, :, fine_span(u), :],
            send_sem=bsend.at[way], recv_sem=brecv.at[z // 2, u],
            **other(row=row, col=y * 2 + parity))

    def b_sent(way):
        return pltpu.make_async_remote_copy(
            src_ref=right.at[:, whole_source, :], dst_ref=bbuf.at[z // 2, c],
            send_sem=bsend.at[way], recv_sem=bown.at[1], **other(**partner))

    b_local = pltpu.make_async_copy(right.at[:, whole_source, :], bbuf.at[z // 2, c], bown.at[0])
    b_partner = b_sent(2)

    def y_part(i):
        return (i == tail).astype(jnp.int32) if not isinstance(i, int) else int(i == tail)

    def y_copy(i):
        return pltpu.make_async_remote_copy(
            src_ref=left.at[:, :, source_span(i)], dst_ref=abuf.at[y, :, :, span(i)],
            send_sem=ysend.at[y_part(i)], recv_sem=yrecv.at[i], **other(**across))

    def y_piece(i):
        return pltpu.make_async_remote_copy(
            src_ref=left.at[:, piece_rows(i), piece_source(i)],
            dst_ref=abuf.at[y, :, piece_rows(i), piece_cols(i)],
            send_sem=ysend.at[y_part(i)], recv_sem=yrecv.at[i], **other(**across))

    def y_sent(part):
        size = (tail if part == 0 else 1) * step
        ref = abuf.at[y, :, :, pl.ds(0, size)]
        return pltpu.make_async_remote_copy(
            src_ref=ref, dst_ref=ref, send_sem=ysend.at[part], recv_sem=yrecv.at[0], **other(**across))

    def y_arrival(i):
        ref = abuf.at[1 - y, :, :, span(i)]
        return pltpu.make_async_copy(ref, ref, yrecv.at[i])

    def y_piece_arrival(i):
        ref = abuf.at[1 - y, :, piece_rows(i), piece_cols(i)]
        return pltpu.make_async_copy(ref, ref, yrecv.at[i])

    def x_own(i):
        return pltpu.make_async_remote_copy(
            src_ref=left.at[:, piece_rows(i), piece_source(i)],
            dst_ref=xbuf.at[:, piece_rows(i), piece_cols(i)],
            send_sem=xsend, recv_sem=xrecv.at[i], **other(row=inward))

    def x_relay(i):
        return pltpu.make_async_remote_copy(
            src_ref=abuf.at[1 - y, :, piece_rows(i), piece_cols(i)],
            dst_ref=xbuf.at[:, piece_rows(i), piece_cols(i)],
            send_sem=xsend, recv_sem=xrecv.at[i], **other(row=inward))

    def x_arrival(i):
        ref = xbuf.at[:, piece_rows(i), piece_cols(i)]
        return pltpu.make_async_copy(ref, ref, xrecv.at[i])

    x_sent = pltpu.make_async_remote_copy(
        src_ref=xbuf, dst_ref=xbuf, send_sem=xsend, recv_sem=xrecv.at[0], **other(row=inward))
    e_own = pltpu.make_async_remote_copy(
        src_ref=left.at[:, :, source_span(tail)], dst_ref=ebuf,
        send_sem=esem.at[0], recv_sem=esem.at[1], **other(row=inward))
    e_relay = pltpu.make_async_remote_copy(
        src_ref=abuf.at[1 - y, :, :, span(tail)], dst_ref=ebuf,
        send_sem=esem.at[0], recv_sem=esem.at[1], **other(row=inward))

    yields = at_end & jnp.logical_not(lends) & (y == lent_slot)
    sends_up = (z < last) & (z != last - 1)
    sends_down = (z > 0) & (z != 1)

    @pl.when(lends_relayed)
    def _():
        y_copy(tail).start()

    def launch(i, carry):
        for k in range(FINE):
            @pl.when(sends_up)
            def _():
                b_copy(i * FINE + k, 0, z + 1).start()

            @pl.when(sends_down)
            def _():
                b_copy(i * FINE + k, 1, z - 1).start()

        @pl.when(jnp.logical_not(yields | lends_own) & jnp.logical_not(lends_relayed & (i == tail)))
        def _():
            y_copy(i).start()

        @pl.when(lends_own)
        def _():
            y_piece(i).start()

        return carry

    lax.fori_loop(0, CHUNKS, launch, 0)

    @pl.when(c == parity)
    def _():
        b_local.start()

    @pl.when(c != parity)
    def _():
        b_partner.start()

    @pl.when(lends_relayed)
    def _():
        e_own.start()

    @pl.when(lends_own)
    def _():
        y_arrival(tail).wait()
        e_relay.start()

        def lend(i, carry):
            x_own(i).start()
            return carry
        lax.fori_loop(0, CHUNKS, lend, 0)
        y_sent(0).wait_send()
        pl.semaphore_signal(turn, inc=1, **other(**partner))

    @pl.when(yields)
    def _():
        pl.semaphore_wait(turn, 1)

        def cross(i, carry):
            y_copy(i).start()
            return carry
        lax.fori_loop(0, CHUNKS, cross, 0)

    own_copy.wait()

    @pl.when(c == parity)
    def _():
        b_local.wait()
        b_sent(2).wait_recv()

    def b_arrival(s, u):
        ref = bbuf.at[s, :, :, fine_span(u), :]
        return pltpu.make_async_copy(ref, ref, brecv.at[s, u])

    def relay(s, u, part, row):
        ref = bbuf.at[s, :, :, fine_span(u), :]
        return pltpu.make_async_remote_copy(
            src_ref=ref, dst_ref=ref, send_sem=rsend.at[s, part], recv_sem=brecv.at[s, u],
            **other(row=row))

    def relayed(s, part):
        start, size = ((0, tail) if part == 0 else (tail, 1))
        ref = bbuf.at[s, :, :, pl.ds(start * step, size * step), :]
        return pltpu.make_async_remote_copy(
            src_ref=ref, dst_ref=ref, send_sem=rsend.at[s, part], recv_sem=brecv.at[s, 0],
            **other(row=inward))

    def present(s):
        quarter = 2 * s + c
        return jnp.logical_not((at_low & (quarter == 1)) | (at_high & (quarter == last - 1)))

    def is_own(s):
        return 2 * s + c == z

    def is_far(s):
        return 2 * s + c == far

    def goes_up(s):
        quarter = 2 * s + c
        return (quarter < z) & (z < last)

    def goes_down(s):
        quarter = 2 * s + c
        return (quarter > z) & (z > 0)

    def goes(s, i):
        cut = is_far(s) & ((z == 1) | (z == last - 1)) & (i == tail)
        return (goes_up(s) | goes_down(s)) & jnp.logical_not(cut)

    def split(value):
        high = value.astype(jnp.bfloat16)
        return high, (value - high.astype(jnp.float32)).astype(jnp.bfloat16)

    def dot(a, b):
        a_high, a_low = split(a)
        b_high, b_low = split(b)
        return jnp.dot(
            jnp.concatenate([a_high, a_high, a_low], axis=1),
            jnp.concatenate([b_high, b_low, b_high], axis=0),
            preferred_element_type=jnp.float32)

    def both(s, at):
        return (jnp.concatenate([bbuf[s, h, k, at, :] for h in range(2)], axis=1) for k in range(2))

    def multiply(a_ref, s, i):
        def add(at):
            a_re, a_im = a_ref[0, :, at], a_ref[1, :, at]
            b_re, b_im = both(s, at)
            acc[0] += dot(a_re, b_re)
            acc[1] += dot(a_im, b_im)
            acc[2] += dot(a_re + a_im, b_re + b_im)

        alone = at_end & is_far(s) & (i == tail)

        @pl.when((i % 2 == 1) & jnp.logical_not(alone))
        def _():
            add(pl.ds(pl.multiple_of((i - 1) * step, 2 * step), 2 * step))

        @pl.when(alone)
        def _():
            add(span(i - 1))

    def lent_multiply(i):
        at, band = piece_cols(i), piece_rows(i)
        a_re, a_im = xbuf[0, band, at], xbuf[1, band, at]
        b_re, b_im = both(z // 2, at)
        xacc[0, band] += dot(a_re, b_re)
        xacc[1, band] += dot(a_im, b_im)
        xacc[2, band] += dot(a_re + a_im, b_re + b_im)

    def right_step(i):
        for s in range(2):
            @pl.when(present(s) & jnp.logical_not(is_own(s)) & jnp.logical_not(at_end & is_far(s) & (i == tail)))
            def _():
                for k in range(FINE):
                    b_arrival(s, i * FINE + k).wait()

                    @pl.when(goes(s, i))
                    def _():
                        relay(s, i * FINE + k, (i == tail).astype(jnp.int32),
                              jnp.where(goes_up(s), z + 1, z - 1)).start()

        @pl.when(present(y))
        def _():
            multiply(abuf.at[y], y, i)

    def left_step(i):
        @pl.when(jnp.logical_not(lends_relayed | (lends_own & (i == tail))))
        def _():
            y_arrival(i).wait()

        @pl.when(lends_relayed)
        def _():
            y_piece_arrival(i).wait()
            x_relay(i).start()

        @pl.when(present(1 - y))
        def _():
            multiply(abuf.at[1 - y], 1 - y, i)

        @pl.when(helps)
        def _():
            x_arrival(i).wait()
            lent_multiply(i)

    early = jnp.logical_not(at_end) & (c != parity)

    def work(t, carry):
        first = t < CHUNKS
        apart = jnp.where(first, t, t - CHUNKS)
        i = jnp.where(early | lends_relayed, apart, t // 2)
        is_left = ((early & jnp.logical_not(first)) | (lends_relayed & first)
                   | (jnp.logical_not(early | lends_relayed) & (t % 2 == 1)))

        @pl.when(is_left)
        def _():
            left_step(i)

        @pl.when(jnp.logical_not(is_left))
        def _():
            right_step(i)

        return carry

    lax.fori_loop(0, 2 * CHUNKS, work, 0)

    def combined(totals, h, g):
        first, second, third = (totals[k, group(g), half(h)] for k in range(3))
        return first - second, third - first - second

    def lend_back(h, g):
        return pltpu.make_async_remote_copy(
            src_ref=xout.at[h, :, group(g)], dst_ref=xin.at[:, group(g)],
            send_sem=csend.at[h], recv_sem=crecv.at[g], **other(row=outward, col=y * 2 + h))

    def lent_back(h):
        return pltpu.make_async_remote_copy(
            src_ref=xout.at[h], dst_ref=xin, send_sem=csend.at[h], recv_sem=crecv.at[0],
            **other(row=outward, col=y * 2 + h))

    def lent_arrival(g):
        ref = xin.at[:, group(g)]
        return pltpu.make_async_copy(ref, ref, crecv.at[g])

    @pl.when(helps)
    def _():
        e_own.wait_recv()
        at = span(tail)

        def give(g, carry):
            band = group(g)
            a_re, a_im = ebuf[0, band, :], ebuf[1, band, :]
            b_re, b_im = both(1 - z // 2, at)
            xacc[0, band] += dot(a_re, b_re)
            xacc[1, band] += dot(a_im, b_im)
            xacc[2, band] += dot(a_re + a_im, b_re + b_im)
            for h in range(2):
                xout[h, 0, band], xout[h, 1, band] = combined(xacc, h, g)
            for h in range(2):
                lend_back(h, g).start()
            return carry

        lax.fori_loop(0, GROUPS, give, 0)

    def to_partner(g):
        return pltpu.make_async_remote_copy(
            src_ref=pout.at[:, group(g)], dst_ref=pin.at[:, group(g)],
            send_sem=psend, recv_sem=precv.at[g], **other(**partner))

    def to_copy(g):
        return pltpu.make_async_remote_copy(
            src_ref=qout.at[:, group(g)], dst_ref=qin.at[:, group(g)],
            send_sem=qsend, recv_sem=qrecv.at[g], **other(**copy_x))

    def hand(g, carry):
        pout[0, group(g)], pout[1, group(g)] = combined(acc, 1 - c, g)
        to_partner(g).start()
        return carry

    lax.fori_loop(0, GROUPS, hand, 0)

    def gather(g, carry):
        band = group(g)
        mine_re, mine_im = combined(acc, c, g)
        to_partner(g).wait_recv()
        qout[0, band] = mine_re + pin[0, band]
        qout[1, band] = mine_im + pin[1, band]

        @pl.when(at_end)
        def _():
            lent_arrival(g).wait()
            qout[:, band] += xin[:, band]

        to_copy(g).start()
        return carry

    lax.fori_loop(0, GROUPS, gather, 0)

    @pl.when(sends_up)
    def _():
        b_sent(0).wait_send()

    @pl.when(sends_down)
    def _():
        b_sent(1).wait_send()

    @pl.when(c != parity)
    def _():
        b_partner.wait_send()

    @pl.when(jnp.logical_not(lends_own))
    def _():
        y_sent(0).wait_send()

    y_sent(1).wait_send()

    @pl.when(lends)
    def _():
        x_sent.wait_send()
        e_own.wait_send()

    for s in range(2):
        for part in range(2):
            @pl.when(present(s) & goes(s, tail * part))
            def _():
                relayed(s, part).wait_send()

    @pl.when(helps)
    def _():
        for h in range(2):
            lent_back(h).wait_send()

    whole_part = pltpu.make_async_remote_copy(
        src_ref=pout, dst_ref=pin, send_sem=psend, recv_sem=precv.at[0], **other(**partner))
    whole_part.wait_send()

    def finish(g, carry):
        to_copy(g).wait_recv()
        band = group(g)
        out[:, band] = qout[:, band] + qin[:, band]
        return carry

    lax.fori_loop(0, GROUPS, finish, 0)
    whole_copy = pltpu.make_async_remote_copy(
        src_ref=qout, dst_ref=qin, send_sem=qsend, recv_sem=qrecv.at[0], **other(**copy_x))
    whole_copy.wait_send()


def lent_product(left_matrix, right_matrix, layers, rows):
    height = left_matrix.shape[1]
    width = right_matrix.shape[2]
    share = left_matrix.shape[2] // layers
    f32 = jnp.float32
    dma = pltpu.SemaphoreType.DMA
    block = (2, height, width)
    return pl.pallas_call(
        functools.partial(kernel, rows),
        out_shape=jax.ShapeDtypeStruct(block, f32),
        in_specs=[pl.BlockSpec(memory_space=pl.ANY)] * 2,
        out_specs=pl.BlockSpec(memory_space=pltpu.VMEM),
        scratch_shapes=[
            pltpu.VMEM((2, 2, height, share), f32),
            pltpu.VMEM((2, 2, 2, share, width), f32),
            pltpu.VMEM((2, height, share), f32),
            pltpu.VMEM((2, height, share // CHUNKS), f32),
            pltpu.VMEM((3, height, 2 * width), f32),
            pltpu.VMEM((3, height, 2 * width), f32),
            pltpu.VMEM((2,) + block, f32),
            pltpu.VMEM(block, f32),
            pltpu.VMEM(block, f32),
            pltpu.VMEM(block, f32),
            pltpu.VMEM(block, f32),
            pltpu.VMEM(block, f32),
            dma,
            dma((3,)),
            dma((2, 2)),
            dma((2, CHUNKS * FINE)),
            dma((2,)),
            dma((2,)),
            dma((CHUNKS,)),
            dma,
            dma((CHUNKS,)),
            dma((2,)),
            dma((2,)),
            dma((GROUPS,)),
            dma,
            dma((GROUPS,)),
            dma,
            dma((GROUPS,)),
            pltpu.SemaphoreType.REGULAR,
        ],
        compiler_params=pltpu.CompilerParams(
            collective_id=0, has_side_effects=True, vmem_limit_bytes=60 * 2**20),
    )(left_matrix, right_matrix)


def gathered_product(left_matrix, right_matrix, layers):
    layer_index = lax.axis_index("layer")
    local_cols = right_matrix.shape[2]
    left_width = left_matrix.shape[2]
    right_height = right_matrix.shape[1]
    share_width = left_width // layers
    group_count = right_height // left_width
    left_own = lax.dynamic_slice_in_dim(left_matrix, layer_index * share_width, share_width, 2)
    right_view = right_matrix.reshape(2, group_count, layers, share_width, local_cols)
    right_own = lax.dynamic_slice_in_dim(right_view, layer_index, 1, 2)
    right_own = right_own.reshape(2, group_count * share_width, local_cols)
    right_whole = lax.all_gather(right_own, "row", axis=1, tiled=True)
    left_whole = lax.all_gather(left_own, "col", axis=2, tiled=True)
    dot = functools.partial(
        jnp.dot, precision=lax.Precision.HIGHEST, preferred_element_type=jnp.float32)
    first_term = dot(left_whole[0], right_whole[0])
    second_term = dot(left_whole[1], right_whole[1])
    third_term = dot(left_whole[0] + left_whole[1], right_whole[0] + right_whole[1])
    partial_product = jnp.stack([first_term - second_term, third_term - first_term - second_term])
    return lax.psum(partial_product, "layer")


def local(left_matrix, right_matrix):
    layers = lax.axis_size("layer")
    rows = lax.axis_size("row")
    cols = lax.axis_size("col")
    if layers == 2 and rows == cols == 4:
        return lent_product(left_matrix, right_matrix, layers, rows)
    return gathered_product(left_matrix, right_matrix, layers)


def solution(mesh):
    in_specs = (P(None, "row", "col"), P(None, "row", "col"))
    out_specs = P(None, "row", "col")
    return jax.shard_map(local, mesh=mesh, in_specs=in_specs, out_specs=out_specs, check_vma=False)
```

```python
import functools

import jax
import jax.numpy as jnp
from jax import lax
from jax.experimental import pallas as pl
from jax.experimental.pallas import tpu as pltpu
from jax.sharding import PartitionSpec as P

CHUNKS = 16
FINE = 2
GROUPS = 4
MESH = pl.DeviceIdType.MESH


def kernel(rows, left, right, own_out, qin, abuf, bbuf, xbuf, ebuf, acc, xacc, xout, xin, pout, pin, qout,
           own_sem, bsend, rsend, brecv, bown, ysend, yrecv, xsend, xrecv, esem, csend, crecv,
           psend, precv, qsend, qrecv, qsave, turn):
    x = lax.axis_index("layer")
    z = lax.axis_index("row")
    col = lax.axis_index("col")
    y = col // 2
    c = col % 2
    height = left.shape[1]
    width = right.shape[2]
    share = abuf.shape[3]
    step = share // CHUNKS
    fine = step // FINE
    tall = height // GROUPS
    wide = share // GROUPS
    last = rows - 1
    tail = CHUNKS - 1
    base = x * share
    parity = z % 2
    at_low, at_high = z == 0, z == last
    at_end = at_low | at_high
    lends = (at_low & (c == 1)) | (at_high & (c == 0))
    helps = ((z == 1) & (c == 1)) | ((z == last - 1) & (c == 0))
    inward = jnp.where(at_low, 1, last - 1)
    outward = jnp.where(z == 1, 0, last)
    far = jnp.where(z < rows // 2, last, 0)
    lent_slot = jnp.where(at_low, 0, (last - 1) // 2)
    lends_own = lends & (y == lent_slot)
    lends_relayed = lends & (y != lent_slot)

    def other(**where):
        return dict(device_id=where, device_id_type=MESH)

    partner = dict(col=y * 2 + 1 - c)
    across = dict(col=(1 - y) * 2 + c)
    copy_x = dict(layer=1 - x)

    barrier = pltpu.get_barrier_semaphore()
    for where in (partner, across, copy_x):
        pl.semaphore_signal(barrier, inc=1, **other(**where))

    @pl.when(z > 0)
    def _():
        for core in range(2):
            pl.semaphore_signal(barrier, inc=1, **other(row=z - 1, col=y * 2 + core))

    @pl.when(z < last)
    def _():
        for core in range(2):
            pl.semaphore_signal(barrier, inc=1, **other(row=z + 1, col=y * 2 + core))

    own_copy = pltpu.make_async_copy(left.at[:, :, pl.ds(base, share)], abuf.at[y], own_sem)
    own_copy.start()
    acc[...] = jnp.zeros_like(acc)
    xacc[...] = jnp.zeros_like(xacc)
    pl.semaphore_wait(barrier, 3 + 2 * ((z > 0).astype(jnp.int32) + (z < last).astype(jnp.int32)))

    def span(i):
        return pl.ds(pl.multiple_of(i * step, step), step)

    def source_span(i):
        return pl.ds(pl.multiple_of(base + i * step, step), step)

    def fine_span(u):
        return pl.ds(pl.multiple_of(u * fine, fine), fine)

    def fine_source(u):
        return pl.ds(pl.multiple_of(base + u * fine, fine), fine)

    def half(h):
        return pl.ds(pl.multiple_of(h * width, width), width)

    def group(g):
        return pl.ds(pl.multiple_of(g * tall, tall), tall)

    def piece_rows(i):
        return group(i // GROUPS)

    def piece_cols(i):
        return pl.ds(pl.multiple_of((i % GROUPS) * wide, wide), wide)

    def piece_source(i):
        return pl.ds(pl.multiple_of(base + (i % GROUPS) * wide, step), wide)

    whole_source = pl.ds(pl.multiple_of(base, step), share)

    def b_copy(u, way, row):
        return pltpu.make_async_remote_copy(
            src_ref=right.at[:, fine_source(u), :],
            dst_ref=bbuf.at[z // 2, c, :, fine_span(u), :],
            send_sem=bsend.at[way], recv_sem=brecv.at[z // 2, u],
            **other(row=row, col=y * 2 + parity))

    def b_sent(way):
        return pltpu.make_async_remote_copy(
            src_ref=right.at[:, whole_source, :], dst_ref=bbuf.at[z // 2, c],
            send_sem=bsend.at[way], recv_sem=bown.at[1], **other(**partner))

    b_local = pltpu.make_async_copy(right.at[:, whole_source, :], bbuf.at[z // 2, c], bown.at[0])
    b_partner = b_sent(2)

    def y_part(i):
        return (i == tail).astype(jnp.int32) if not isinstance(i, int) else int(i == tail)

    def y_copy(i):
        return pltpu.make_async_remote_copy(
            src_ref=left.at[:, :, source_span(i)], dst_ref=abuf.at[y, :, :, span(i)],
            send_sem=ysend.at[y_part(i)], recv_sem=yrecv.at[i], **other(**across))

    def y_piece(i):
        return pltpu.make_async_remote_copy(
            src_ref=left.at[:, piece_rows(i), piece_source(i)],
            dst_ref=abuf.at[y, :, piece_rows(i), piece_cols(i)],
            send_sem=ysend.at[y_part(i)], recv_sem=yrecv.at[i], **other(**across))

    def y_sent(part):
        size = (tail if part == 0 else 1) * step
        ref = abuf.at[y, :, :, pl.ds(0, size)]
        return pltpu.make_async_remote_copy(
            src_ref=ref, dst_ref=ref, send_sem=ysend.at[part], recv_sem=yrecv.at[0], **other(**across))

    def y_arrival(i):
        ref = abuf.at[1 - y, :, :, span(i)]
        return pltpu.make_async_copy(ref, ref, yrecv.at[i])

    def y_piece_arrival(i):
        ref = abuf.at[1 - y, :, piece_rows(i), piece_cols(i)]
        return pltpu.make_async_copy(ref, ref, yrecv.at[i])

    def x_own(i):
        return pltpu.make_async_remote_copy(
            src_ref=left.at[:, piece_rows(i), piece_source(i)],
            dst_ref=xbuf.at[:, piece_rows(i), piece_cols(i)],
            send_sem=xsend, recv_sem=xrecv.at[i], **other(row=inward))

    def x_relay(i):
        return pltpu.make_async_remote_copy(
            src_ref=abuf.at[1 - y, :, piece_rows(i), piece_cols(i)],
            dst_ref=xbuf.at[:, piece_rows(i), piece_cols(i)],
            send_sem=xsend, recv_sem=xrecv.at[i], **other(row=inward))

    def x_arrival(i):
        ref = xbuf.at[:, piece_rows(i), piece_cols(i)]
        return pltpu.make_async_copy(ref, ref, xrecv.at[i])

    x_sent = pltpu.make_async_remote_copy(
        src_ref=xbuf, dst_ref=xbuf, send_sem=xsend, recv_sem=xrecv.at[0], **other(row=inward))
    e_own = pltpu.make_async_remote_copy(
        src_ref=left.at[:, :, source_span(tail)], dst_ref=ebuf,
        send_sem=esem.at[0], recv_sem=esem.at[1], **other(row=inward))
    e_relay = pltpu.make_async_remote_copy(
        src_ref=abuf.at[1 - y, :, :, span(tail)], dst_ref=ebuf,
        send_sem=esem.at[0], recv_sem=esem.at[1], **other(row=inward))

    yields = at_end & jnp.logical_not(lends) & (y == lent_slot)
    sends_up = (z < last) & (z != last - 1)
    sends_down = (z > 0) & (z != 1)

    @pl.when(lends_relayed)
    def _():
        y_copy(tail).start()

    def launch(i, carry):
        for k in range(FINE):
            @pl.when(sends_up)
            def _():
                b_copy(i * FINE + k, 0, z + 1).start()

            @pl.when(sends_down)
            def _():
                b_copy(i * FINE + k, 1, z - 1).start()

        @pl.when(jnp.logical_not(yields | lends_own) & jnp.logical_not(lends_relayed & (i == tail)))
        def _():
            y_copy(i).start()

        @pl.when(lends_own)
        def _():
            y_piece(i).start()

        return carry

    lax.fori_loop(0, CHUNKS, launch, 0)

    @pl.when(c == parity)
    def _():
        b_local.start()

    @pl.when(c != parity)
    def _():
        b_partner.start()

    @pl.when(lends_relayed)
    def _():
        e_own.start()

    @pl.when(lends_own)
    def _():
        y_arrival(tail).wait()
        e_relay.start()

        def lend(i, carry):
            x_own(i).start()
            return carry
        lax.fori_loop(0, CHUNKS, lend, 0)
        y_sent(0).wait_send()
        pl.semaphore_signal(turn, inc=1, **other(**partner))

    @pl.when(yields)
    def _():
        pl.semaphore_wait(turn, 1)

        def cross(i, carry):
            y_copy(i).start()
            return carry
        lax.fori_loop(0, CHUNKS, cross, 0)

    own_copy.wait()

    @pl.when(c == parity)
    def _():
        b_local.wait()
        b_sent(2).wait_recv()

    def b_arrival(s, u):
        ref = bbuf.at[s, :, :, fine_span(u), :]
        return pltpu.make_async_copy(ref, ref, brecv.at[s, u])

    def relay(s, u, part, row):
        ref = bbuf.at[s, :, :, fine_span(u), :]
        return pltpu.make_async_remote_copy(
            src_ref=ref, dst_ref=ref, send_sem=rsend.at[s, part], recv_sem=brecv.at[s, u],
            **other(row=row))

    def relayed(s, part):
        start, size = ((0, tail) if part == 0 else (tail, 1))
        ref = bbuf.at[s, :, :, pl.ds(start * step, size * step), :]
        return pltpu.make_async_remote_copy(
            src_ref=ref, dst_ref=ref, send_sem=rsend.at[s, part], recv_sem=brecv.at[s, 0],
            **other(row=inward))

    def present(s):
        quarter = 2 * s + c
        return jnp.logical_not((at_low & (quarter == 1)) | (at_high & (quarter == last - 1)))

    def is_own(s):
        return 2 * s + c == z

    def is_far(s):
        return 2 * s + c == far

    def goes_up(s):
        quarter = 2 * s + c
        return (quarter < z) & (z < last)

    def goes_down(s):
        quarter = 2 * s + c
        return (quarter > z) & (z > 0)

    def goes(s, i):
        cut = is_far(s) & ((z == 1) | (z == last - 1)) & (i == tail)
        return (goes_up(s) | goes_down(s)) & jnp.logical_not(cut)

    def split(value):
        high = value.astype(jnp.bfloat16)
        return high, (value - high.astype(jnp.float32)).astype(jnp.bfloat16)

    def dot(a, b):
        a_high, a_low = split(a)
        b_high, b_low = split(b)
        return jnp.dot(
            jnp.concatenate([a_high, a_high, a_low], axis=1),
            jnp.concatenate([b_high, b_low, b_high], axis=0),
            preferred_element_type=jnp.float32)

    def both(s, at):
        return (jnp.concatenate([bbuf[s, h, k, at, :] for h in range(2)], axis=1) for k in range(2))

    def multiply(a_ref, s, i):
        def add(at):
            a_re, a_im = a_ref[0, :, at], a_ref[1, :, at]
            b_re, b_im = both(s, at)
            acc[0] += dot(a_re, b_re)
            acc[1] += dot(a_im, b_im)
            acc[2] += dot(a_re + a_im, b_re + b_im)

        alone = at_end & is_far(s) & (i == tail)

        @pl.when((i % 2 == 1) & jnp.logical_not(alone))
        def _():
            add(pl.ds(pl.multiple_of((i - 1) * step, 2 * step), 2 * step))

        @pl.when(alone)
        def _():
            add(span(i - 1))

    def lent_multiply(i):
        at, band = piece_cols(i), piece_rows(i)
        a_re, a_im = xbuf[0, band, at], xbuf[1, band, at]
        b_re, b_im = both(z // 2, at)
        xacc[0, band] += dot(a_re, b_re)
        xacc[1, band] += dot(a_im, b_im)
        xacc[2, band] += dot(a_re + a_im, b_re + b_im)

    def combined(totals, h, g):
        first, second, third = (totals[k, group(g), half(h)] for k in range(3))
        return first - second, third - first - second

    def lend_back(h, g):
        return pltpu.make_async_remote_copy(
            src_ref=xout.at[h, :, group(g)], dst_ref=xin.at[:, group(g)],
            send_sem=csend.at[h], recv_sem=crecv.at[g], **other(row=outward, col=y * 2 + h))

    def lent_back(h):
        return pltpu.make_async_remote_copy(
            src_ref=xout.at[h], dst_ref=xin, send_sem=csend.at[h], recv_sem=crecv.at[0],
            **other(row=outward, col=y * 2 + h))

    def lent_arrival(g):
        ref = xin.at[:, group(g)]
        return pltpu.make_async_copy(ref, ref, crecv.at[g])

    def give(g, carry):
        for h in range(2):
            xout[h, 0, group(g)], xout[h, 1, group(g)] = combined(xacc, h, g)
        for h in range(2):
            lend_back(h, g).start()
        return carry

    def extra_multiply():
        e_own.wait_recv()
        b_re, b_im = both(1 - z // 2, span(tail))
        xacc[0] += dot(ebuf[0], b_re)
        xacc[1] += dot(ebuf[1], b_im)
        xacc[2] += dot(ebuf[0] + ebuf[1], b_re + b_im)
        lax.fori_loop(0, GROUPS - 1, give, 0)

    def right_step(i):
        for s in range(2):
            @pl.when(present(s) & jnp.logical_not(is_own(s)) & jnp.logical_not(at_end & is_far(s) & (i == tail)))
            def _():
                for k in range(FINE):
                    b_arrival(s, i * FINE + k).wait()

                    @pl.when(goes(s, i))
                    def _():
                        relay(s, i * FINE + k, (i == tail).astype(jnp.int32),
                              jnp.where(goes_up(s), z + 1, z - 1)).start()

        @pl.when(helps & (i == tail))
        def _():
            extra_multiply()

        @pl.when(present(y))
        def _():
            multiply(abuf.at[y], y, i)

    def left_step(i):
        @pl.when(jnp.logical_not(lends_relayed | (lends_own & (i == tail))))
        def _():
            y_arrival(i).wait()

        @pl.when(lends_relayed)
        def _():
            y_piece_arrival(i).wait()
            x_relay(i).start()

        @pl.when(present(1 - y))
        def _():
            multiply(abuf.at[1 - y], 1 - y, i)

        @pl.when(helps)
        def _():
            x_arrival(i).wait()
            lent_multiply(i)

            @pl.when(i == tail)
            def _():
                give(GROUPS - 1, 0)

    early = jnp.logical_not(at_end) & (c != parity)

    def work(t, carry):
        first = t < CHUNKS
        apart = jnp.where(first, t, t - CHUNKS)
        i = jnp.where(early | lends_relayed, apart, t // 2)
        is_left = ((early & jnp.logical_not(first)) | (lends_relayed & first)
                   | (jnp.logical_not(early | lends_relayed) & (t % 2 == 1)))

        @pl.when(is_left)
        def _():
            left_step(i)

        @pl.when(jnp.logical_not(is_left))
        def _():
            right_step(i)

        return carry

    lax.fori_loop(0, 2 * CHUNKS, work, 0)

    def to_partner(g):
        return pltpu.make_async_remote_copy(
            src_ref=pout.at[:, group(g)], dst_ref=pin.at[:, group(g)],
            send_sem=psend, recv_sem=precv.at[g], **other(**partner))

    def to_copy(g):
        return pltpu.make_async_remote_copy(
            src_ref=qout.at[:, group(g)], dst_ref=qin.at[:, group(g)],
            send_sem=qsend, recv_sem=qrecv, **other(**copy_x))

    def keep(g):
        return pltpu.make_async_copy(qout.at[:, group(g)], own_out.at[:, group(g)], qsave)

    def hand(g, carry):
        pout[0, group(g)], pout[1, group(g)] = combined(acc, 1 - c, g)
        to_partner(g).start()
        return carry

    lax.fori_loop(0, GROUPS, hand, 0)

    def gather(g, carry):
        band = group(g)
        mine_re, mine_im = combined(acc, c, g)
        to_partner(g).wait_recv()
        qout[0, band] = mine_re + pin[0, band]
        qout[1, band] = mine_im + pin[1, band]

        @pl.when(at_end)
        def _():
            lent_arrival(g).wait()
            qout[:, band] += xin[:, band]

        to_copy(g).start()
        keep(g).start()
        return carry

    lax.fori_loop(0, GROUPS, gather, 0)

    @pl.when(sends_up)
    def _():
        b_sent(0).wait_send()

    @pl.when(sends_down)
    def _():
        b_sent(1).wait_send()

    @pl.when(c != parity)
    def _():
        b_partner.wait_send()

    @pl.when(jnp.logical_not(lends_own))
    def _():
        y_sent(0).wait_send()

    y_sent(1).wait_send()

    @pl.when(lends)
    def _():
        x_sent.wait_send()
        e_own.wait_send()

    for s in range(2):
        for part in range(2):
            @pl.when(present(s) & goes(s, tail * part))
            def _():
                relayed(s, part).wait_send()

    @pl.when(helps)
    def _():
        for h in range(2):
            lent_back(h).wait_send()

    whole_part = pltpu.make_async_remote_copy(
        src_ref=pout, dst_ref=pin, send_sem=psend, recv_sem=precv.at[0], **other(**partner))
    whole_part.wait_send()

    pltpu.make_async_copy(qout, own_out, qsave).wait()
    whole_copy = pltpu.make_async_remote_copy(
        src_ref=qout, dst_ref=qin, send_sem=qsend, recv_sem=qrecv, **other(**copy_x))
    whole_copy.wait()


def lent_product(left_matrix, right_matrix, layers, rows):
    height = left_matrix.shape[1]
    width = right_matrix.shape[2]
    share = left_matrix.shape[2] // layers
    f32 = jnp.float32
    dma = pltpu.SemaphoreType.DMA
    block = (2, height, width)
    own, copied = pl.pallas_call(
        functools.partial(kernel, rows),
        out_shape=[jax.ShapeDtypeStruct(block, f32)] * 2,
        in_specs=[pl.BlockSpec(memory_space=pl.ANY)] * 2,
        out_specs=[pl.BlockSpec(memory_space=pl.ANY)] * 2,
        scratch_shapes=[
            pltpu.VMEM((2, 2, height, share), f32),
            pltpu.VMEM((2, 2, 2, share, width), f32),
            pltpu.VMEM((2, height, share), f32),
            pltpu.VMEM((2, height, share // CHUNKS), f32),
            pltpu.VMEM((3, height, 2 * width), f32),
            pltpu.VMEM((3, height, 2 * width), f32),
            pltpu.VMEM((2,) + block, f32),
            pltpu.VMEM(block, f32),
            pltpu.VMEM(block, f32),
            pltpu.VMEM(block, f32),
            pltpu.VMEM(block, f32),
            dma,
            dma((3,)),
            dma((2, 2)),
            dma((2, CHUNKS * FINE)),
            dma((2,)),
            dma((2,)),
            dma((CHUNKS,)),
            dma,
            dma((CHUNKS,)),
            dma((2,)),
            dma((2,)),
            dma((GROUPS,)),
            dma,
            dma((GROUPS,)),
            dma,
            dma,
            dma,
            pltpu.SemaphoreType.REGULAR,
        ],
        compiler_params=pltpu.CompilerParams(
            collective_id=0, has_side_effects=True, vmem_limit_bytes=60 * 2**20),
    )(left_matrix, right_matrix)
    return own + copied


def gathered_product(left_matrix, right_matrix, layers):
    layer_index = lax.axis_index("layer")
    local_cols = right_matrix.shape[2]
    left_width = left_matrix.shape[2]
    right_height = right_matrix.shape[1]
    share_width = left_width // layers
    group_count = right_height // left_width
    left_own = lax.dynamic_slice_in_dim(left_matrix, layer_index * share_width, share_width, 2)
    right_view = right_matrix.reshape(2, group_count, layers, share_width, local_cols)
    right_own = lax.dynamic_slice_in_dim(right_view, layer_index, 1, 2)
    right_own = right_own.reshape(2, group_count * share_width, local_cols)
    right_whole = lax.all_gather(right_own, "row", axis=1, tiled=True)
    left_whole = lax.all_gather(left_own, "col", axis=2, tiled=True)
    dot = functools.partial(
        jnp.dot, precision=lax.Precision.HIGHEST, preferred_element_type=jnp.float32)
    first_term = dot(left_whole[0], right_whole[0])
    second_term = dot(left_whole[1], right_whole[1])
    third_term = dot(left_whole[0] + left_whole[1], right_whole[0] + right_whole[1])
    partial_product = jnp.stack([first_term - second_term, third_term - first_term - second_term])
    return lax.psum(partial_product, "layer")


def local(left_matrix, right_matrix):
    layers = lax.axis_size("layer")
    rows = lax.axis_size("row")
    cols = lax.axis_size("col")
    if layers == 2 and rows == cols == 4:
        return lent_product(left_matrix, right_matrix, layers, rows)
    return gathered_product(left_matrix, right_matrix, layers)


def solution(mesh):
    in_specs = (P(None, "row", "col"), P(None, "row", "col"))
    out_specs = P(None, "row", "col")
    return jax.shard_map(local, mesh=mesh, in_specs=in_specs, out_specs=out_specs, check_vma=False)
```

```python
import functools

import jax
import jax.numpy as jnp
from jax import lax
from jax.experimental import pallas as pl
from jax.experimental.pallas import tpu as pltpu
from jax.sharding import PartitionSpec as P

CHUNKS = 16
FINE = 2
GROUPS = 4
LAG = 2
BANDS = 8
MESH = pl.DeviceIdType.MESH


def kernel(rows, left, right, qout, qin, abuf, bbuf, xbuf, ebuf, acc, xacc, xout, xin, pout, pin,
           own_sem, bsend, rsend, brecv, bown, ysend, yrecv, xsend, xrecv, esem, csend, crecv,
           psend, precv, qsend, qrecv, turn):
    x = lax.axis_index("layer")
    z = lax.axis_index("row")
    col = lax.axis_index("col")
    y = col // 2
    c = col % 2
    height = left.shape[1]
    width = right.shape[2]
    share = abuf.shape[3]
    step = share // CHUNKS
    fine = step // FINE
    tall = height // GROUPS
    wide = share // GROUPS
    last = rows - 1
    tail = CHUNKS - 1
    base = x * share
    parity = z % 2
    at_low, at_high = z == 0, z == last
    at_end = at_low | at_high
    lends = (at_low & (c == 1)) | (at_high & (c == 0))
    helps = ((z == 1) & (c == 1)) | ((z == last - 1) & (c == 0))
    inward = jnp.where(at_low, 1, last - 1)
    outward = jnp.where(z == 1, 0, last)
    far = jnp.where(z < rows // 2, last, 0)
    lent_slot = jnp.where(at_low, 0, (last - 1) // 2)
    lends_own = lends & (y == lent_slot)
    lends_relayed = lends & (y != lent_slot)

    def other(**where):
        return dict(device_id=where, device_id_type=MESH)

    partner = dict(col=y * 2 + 1 - c)
    across = dict(col=(1 - y) * 2 + c)
    copy_x = dict(layer=1 - x)

    barrier = pltpu.get_barrier_semaphore()
    for where in (partner, across, copy_x):
        pl.semaphore_signal(barrier, inc=1, **other(**where))

    @pl.when(z > 0)
    def _():
        for core in range(2):
            pl.semaphore_signal(barrier, inc=1, **other(row=z - 1, col=y * 2 + core))

    @pl.when(z < last)
    def _():
        for core in range(2):
            pl.semaphore_signal(barrier, inc=1, **other(row=z + 1, col=y * 2 + core))

    own_copy = pltpu.make_async_copy(left.at[:, :, pl.ds(base, share)], abuf.at[y], own_sem)
    own_copy.start()
    acc[...] = jnp.zeros_like(acc)
    xacc[...] = jnp.zeros_like(xacc)
    pl.semaphore_wait(barrier, 3 + 2 * ((z > 0).astype(jnp.int32) + (z < last).astype(jnp.int32)))

    def span(i):
        return pl.ds(pl.multiple_of(i * step, step), step)

    def source_span(i):
        return pl.ds(pl.multiple_of(base + i * step, step), step)

    def fine_span(u):
        return pl.ds(pl.multiple_of(u * fine, fine), fine)

    def fine_source(u):
        return pl.ds(pl.multiple_of(base + u * fine, fine), fine)

    def half(h):
        return pl.ds(pl.multiple_of(h * width, width), width)

    def group(g):
        return pl.ds(pl.multiple_of(g * tall, tall), tall)

    def piece_rows(i):
        return group(i // GROUPS)

    def piece_cols(i):
        return pl.ds(pl.multiple_of((i % GROUPS) * wide, wide), wide)

    def piece_source(i):
        return pl.ds(pl.multiple_of(base + (i % GROUPS) * wide, step), wide)

    whole_source = pl.ds(pl.multiple_of(base, step), share)

    def b_copy(u, way, row):
        return pltpu.make_async_remote_copy(
            src_ref=right.at[:, fine_source(u), :],
            dst_ref=bbuf.at[z // 2, c, :, fine_span(u), :],
            send_sem=bsend.at[way], recv_sem=brecv.at[z // 2, u],
            **other(row=row, col=y * 2 + parity))

    def b_sent(way):
        return pltpu.make_async_remote_copy(
            src_ref=right.at[:, whole_source, :], dst_ref=bbuf.at[z // 2, c],
            send_sem=bsend.at[way], recv_sem=bown.at[1], **other(**partner))

    b_local = pltpu.make_async_copy(right.at[:, whole_source, :], bbuf.at[z // 2, c], bown.at[0])
    b_partner = b_sent(2)

    def y_part(i):
        return (i == tail).astype(jnp.int32) if not isinstance(i, int) else int(i == tail)

    def y_copy(i):
        return pltpu.make_async_remote_copy(
            src_ref=left.at[:, :, source_span(i)], dst_ref=abuf.at[y, :, :, span(i)],
            send_sem=ysend.at[y_part(i)], recv_sem=yrecv.at[i], **other(**across))

    def y_piece(i):
        return pltpu.make_async_remote_copy(
            src_ref=left.at[:, piece_rows(i), piece_source(i)],
            dst_ref=abuf.at[y, :, piece_rows(i), piece_cols(i)],
            send_sem=ysend.at[y_part(i)], recv_sem=yrecv.at[i], **other(**across))

    def y_sent(part):
        size = (tail if part == 0 else 1) * step
        ref = abuf.at[y, :, :, pl.ds(0, size)]
        return pltpu.make_async_remote_copy(
            src_ref=ref, dst_ref=ref, send_sem=ysend.at[part], recv_sem=yrecv.at[0], **other(**across))

    def y_arrival(i):
        ref = abuf.at[1 - y, :, :, span(i)]
        return pltpu.make_async_copy(ref, ref, yrecv.at[i])

    def y_piece_arrival(i):
        ref = abuf.at[1 - y, :, piece_rows(i), piece_cols(i)]
        return pltpu.make_async_copy(ref, ref, yrecv.at[i])

    def x_own(i):
        return pltpu.make_async_remote_copy(
            src_ref=left.at[:, piece_rows(i), piece_source(i)],
            dst_ref=xbuf.at[:, piece_rows(i), piece_cols(i)],
            send_sem=xsend, recv_sem=xrecv.at[i], **other(row=inward))

    def x_relay(i):
        return pltpu.make_async_remote_copy(
            src_ref=abuf.at[1 - y, :, piece_rows(i), piece_cols(i)],
            dst_ref=xbuf.at[:, piece_rows(i), piece_cols(i)],
            send_sem=xsend, recv_sem=xrecv.at[i], **other(row=inward))

    def x_arrival(i):
        ref = xbuf.at[:, piece_rows(i), piece_cols(i)]
        return pltpu.make_async_copy(ref, ref, xrecv.at[i])

    x_sent = pltpu.make_async_remote_copy(
        src_ref=xbuf, dst_ref=xbuf, send_sem=xsend, recv_sem=xrecv.at[0], **other(row=inward))
    e_own = pltpu.make_async_remote_copy(
        src_ref=left.at[:, :, source_span(tail)], dst_ref=ebuf,
        send_sem=esem.at[0], recv_sem=esem.at[1], **other(row=inward))
    e_relay = pltpu.make_async_remote_copy(
        src_ref=abuf.at[1 - y, :, :, span(tail)], dst_ref=ebuf,
        send_sem=esem.at[0], recv_sem=esem.at[1], **other(row=inward))

    yields = at_end & jnp.logical_not(lends) & (y == lent_slot)
    sends_up = (z < last) & (z != last - 1)
    sends_down = (z > 0) & (z != 1)

    @pl.when(lends_relayed)
    def _():
        y_copy(tail).start()

    def launch(i, carry):
        for k in range(FINE):
            @pl.when(sends_up)
            def _():
                b_copy(i * FINE + k, 0, z + 1).start()

            @pl.when(sends_down)
            def _():
                b_copy(i * FINE + k, 1, z - 1).start()

        @pl.when(jnp.logical_not(yields | lends_own) & jnp.logical_not(lends_relayed & (i == tail)))
        def _():
            y_copy(i).start()

        @pl.when(lends_own)
        def _():
            y_piece(i).start()

        return carry

    lax.fori_loop(0, CHUNKS, launch, 0)

    @pl.when(c == parity)
    def _():
        b_local.start()

    @pl.when(c != parity)
    def _():
        b_partner.start()

    @pl.when(lends_relayed)
    def _():
        e_own.start()

    @pl.when(lends_own)
    def _():
        y_arrival(tail).wait()
        e_relay.start()

        def lend(i, carry):
            x_own(i).start()
            return carry
        lax.fori_loop(0, CHUNKS, lend, 0)
        y_sent(0).wait_send()
        pl.semaphore_signal(turn, inc=1, **other(**partner))

    @pl.when(yields)
    def _():
        pl.semaphore_wait(turn, 1)

        def cross(i, carry):
            y_copy(i).start()
            return carry
        lax.fori_loop(0, CHUNKS, cross, 0)

    own_copy.wait()

    @pl.when(c == parity)
    def _():
        b_local.wait()
        b_sent(2).wait_recv()

    def b_arrival(s, u):
        ref = bbuf.at[s, :, :, fine_span(u), :]
        return pltpu.make_async_copy(ref, ref, brecv.at[s, u])

    def relay(s, u, part, row):
        ref = bbuf.at[s, :, :, fine_span(u), :]
        return pltpu.make_async_remote_copy(
            src_ref=ref, dst_ref=ref, send_sem=rsend.at[s, part], recv_sem=brecv.at[s, u],
            **other(row=row))

    def relayed(s, part):
        start, size = ((0, tail) if part == 0 else (tail, 1))
        ref = bbuf.at[s, :, :, pl.ds(start * step, size * step), :]
        return pltpu.make_async_remote_copy(
            src_ref=ref, dst_ref=ref, send_sem=rsend.at[s, part], recv_sem=brecv.at[s, 0],
            **other(row=inward))

    def present(s):
        quarter = 2 * s + c
        return jnp.logical_not((at_low & (quarter == 1)) | (at_high & (quarter == last - 1)))

    def is_own(s):
        return 2 * s + c == z

    def is_far(s):
        return 2 * s + c == far

    def goes_up(s):
        quarter = 2 * s + c
        return (quarter < z) & (z < last)

    def goes_down(s):
        quarter = 2 * s + c
        return (quarter > z) & (z > 0)

    def goes(s, i):
        cut = is_far(s) & ((z == 1) | (z == last - 1)) & (i == tail)
        return (goes_up(s) | goes_down(s)) & jnp.logical_not(cut)

    def split(value):
        high = value.astype(jnp.bfloat16)
        return high, (value - high.astype(jnp.float32)).astype(jnp.bfloat16)

    def dot(a, b):
        a_high, a_low = split(a)
        b_high, b_low = split(b)
        return jnp.dot(
            jnp.concatenate([a_high, a_high, a_low], axis=1),
            jnp.concatenate([b_high, b_low, b_high], axis=0),
            preferred_element_type=jnp.float32)

    def both(s, at):
        return (jnp.concatenate([bbuf[s, h, k, at, :] for h in range(2)], axis=1) for k in range(2))

    def multiply(a_ref, s, i):
        def add(at):
            a_re, a_im = a_ref[0, :, at], a_ref[1, :, at]
            b_re, b_im = both(s, at)
            acc[0] += dot(a_re, b_re)
            acc[1] += dot(a_im, b_im)
            acc[2] += dot(a_re + a_im, b_re + b_im)

        alone = at_end & is_far(s) & (i == tail)

        @pl.when((i % 2 == 1) & jnp.logical_not(alone))
        def _():
            add(pl.ds(pl.multiple_of((i - 1) * step, 2 * step), 2 * step))

        @pl.when(alone)
        def _():
            add(span(i - 1))

    def lent_multiply(i):
        at, band = piece_cols(i), piece_rows(i)
        a_re, a_im = xbuf[0, band, at], xbuf[1, band, at]
        b_re, b_im = both(z // 2, at)
        xacc[0, band] += dot(a_re, b_re)
        xacc[1, band] += dot(a_im, b_im)
        xacc[2, band] += dot(a_re + a_im, b_re + b_im)

    def combined(totals, h, g):
        first, second, third = (totals[k, group(g), half(h)] for k in range(3))
        return first - second, third - first - second

    def lend_back(h, g):
        return pltpu.make_async_remote_copy(
            src_ref=xout.at[h, :, group(g)], dst_ref=xin.at[:, group(g)],
            send_sem=csend.at[h], recv_sem=crecv.at[g], **other(row=outward, col=y * 2 + h))

    def lent_back(h):
        return pltpu.make_async_remote_copy(
            src_ref=xout.at[h], dst_ref=xin, send_sem=csend.at[h], recv_sem=crecv.at[0],
            **other(row=outward, col=y * 2 + h))

    def lent_arrival(g):
        ref = xin.at[:, group(g)]
        return pltpu.make_async_copy(ref, ref, crecv.at[g])

    def give(g, carry):
        for h in range(2):
            xout[h, 0, group(g)], xout[h, 1, group(g)] = combined(xacc, h, g)
        for h in range(2):
            lend_back(h, g).start()
        return carry

    def extra_multiply():
        e_own.wait_recv()
        b_re, b_im = both(1 - z // 2, span(tail))
        xacc[0] += dot(ebuf[0], b_re)
        xacc[1] += dot(ebuf[1], b_im)
        xacc[2] += dot(ebuf[0] + ebuf[1], b_re + b_im)
        lax.fori_loop(0, GROUPS - 1, give, 0)

    def right_step(i):
        for s in range(2):
            @pl.when(present(s) & jnp.logical_not(is_own(s)) & jnp.logical_not(at_end & is_far(s) & (i == tail)))
            def _():
                for k in range(FINE):
                    b_arrival(s, i * FINE + k).wait()

                    @pl.when(goes(s, i))
                    def _():
                        relay(s, i * FINE + k, (i == tail).astype(jnp.int32),
                              jnp.where(goes_up(s), z + 1, z - 1)).start()

        @pl.when(helps & (i == tail))
        def _():
            extra_multiply()

        @pl.when(present(y))
        def _():
            multiply(abuf.at[y], y, i)

    def lent_step(i):
        x_arrival(i).wait()
        lent_multiply(i)

    def left_step(i):
        @pl.when(jnp.logical_not(lends_relayed | (lends_own & (i == tail))))
        def _():
            y_arrival(i).wait()

        @pl.when(lends_relayed)
        def _():
            y_piece_arrival(i).wait()
            x_relay(i).start()

        @pl.when(present(1 - y))
        def _():
            multiply(abuf.at[1 - y], 1 - y, i)

        @pl.when(helps & (i >= LAG))
        def _():
            lent_step(i - LAG)

    early = jnp.logical_not(at_end) & (c != parity)

    def work(t, carry):
        first = t < CHUNKS
        apart = jnp.where(first, t, t - CHUNKS)
        i = jnp.where(early | lends_relayed, apart, t // 2)
        is_left = ((early & jnp.logical_not(first)) | (lends_relayed & first)
                   | (jnp.logical_not(early | lends_relayed) & (t % 2 == 1)))

        @pl.when(is_left)
        def _():
            left_step(i)

        @pl.when(jnp.logical_not(is_left))
        def _():
            right_step(i)

        return carry

    lax.fori_loop(0, 2 * CHUNKS, work, 0)

    @pl.when(helps)
    def _():
        def lent_rest(i, carry):
            lent_step(i)
            return carry
        lax.fori_loop(CHUNKS - LAG, CHUNKS, lent_rest, 0)
        give(GROUPS - 1, 0)

    thin = height // BANDS

    def band_of(b):
        return pl.ds(pl.multiple_of(b * thin, thin), thin)

    def banded(h, b):
        first, second, third = (acc[k, band_of(b), half(h)] for k in range(3))
        return first - second, third - first - second

    def to_partner(b):
        return pltpu.make_async_remote_copy(
            src_ref=pout.at[:, band_of(b)], dst_ref=pin.at[:, band_of(b)],
            send_sem=psend, recv_sem=precv.at[b], **other(**partner))

    def to_copy(b):
        return pltpu.make_async_remote_copy(
            src_ref=qout.at[:, band_of(b)], dst_ref=qin.at[:, band_of(b)],
            send_sem=qsend, recv_sem=qrecv, **other(**copy_x))

    def hand(b, carry):
        pout[0, band_of(b)], pout[1, band_of(b)] = banded(1 - c, b)
        to_partner(b).start()
        return carry

    lax.fori_loop(0, BANDS, hand, 0)

    def gather(b, carry):
        band = band_of(b)
        mine_re, mine_im = banded(c, b)
        to_partner(b).wait_recv()
        qout[0, band] = mine_re + pin[0, band]
        qout[1, band] = mine_im + pin[1, band]

        @pl.when(at_end)
        def _():
            @pl.when(b % (BANDS // GROUPS) == 0)
            def _():
                lent_arrival(b // (BANDS // GROUPS)).wait()
            qout[:, band] += xin[:, band]

        to_copy(b).start()
        return carry

    lax.fori_loop(0, BANDS, gather, 0)

    @pl.when(sends_up)
    def _():
        b_sent(0).wait_send()

    @pl.when(sends_down)
    def _():
        b_sent(1).wait_send()

    @pl.when(c != parity)
    def _():
        b_partner.wait_send()

    @pl.when(jnp.logical_not(lends_own))
    def _():
        y_sent(0).wait_send()

    y_sent(1).wait_send()

    @pl.when(lends)
    def _():
        x_sent.wait_send()
        e_own.wait_send()

    for s in range(2):
        for part in range(2):
            @pl.when(present(s) & goes(s, tail * part))
            def _():
                relayed(s, part).wait_send()

    @pl.when(helps)
    def _():
        for h in range(2):
            lent_back(h).wait_send()

    whole_part = pltpu.make_async_remote_copy(
        src_ref=pout, dst_ref=pin, send_sem=psend, recv_sem=precv.at[0], **other(**partner))
    whole_part.wait_send()

    whole_copy = pltpu.make_async_remote_copy(
        src_ref=qout, dst_ref=qin, send_sem=qsend, recv_sem=qrecv, **other(**copy_x))
    whole_copy.wait()


def lent_product(left_matrix, right_matrix, layers, rows):
    height = left_matrix.shape[1]
    width = right_matrix.shape[2]
    share = left_matrix.shape[2] // layers
    f32 = jnp.float32
    dma = pltpu.SemaphoreType.DMA
    block = (2, height, width)
    own, copied = pl.pallas_call(
        functools.partial(kernel, rows),
        out_shape=[pltpu.VMEM(block, f32)] * 2,
        in_specs=[pl.BlockSpec(memory_space=pl.ANY)] * 2,
        out_specs=[pl.BlockSpec(memory_space=pltpu.VMEM)] * 2,
        scratch_shapes=[
            pltpu.VMEM((2, 2, height, share), f32),
            pltpu.VMEM((2, 2, 2, share, width), f32),
            pltpu.VMEM((2, height, share), f32),
            pltpu.VMEM((2, height, share // CHUNKS), f32),
            pltpu.VMEM((3, height, 2 * width), f32),
            pltpu.VMEM((3, height, 2 * width), f32),
            pltpu.VMEM((2,) + block, f32),
            pltpu.VMEM(block, f32),
            pltpu.VMEM(block, f32),
            pltpu.VMEM(block, f32),
            dma,
            dma((3,)),
            dma((2, 2)),
            dma((2, CHUNKS * FINE)),
            dma((2,)),
            dma((2,)),
            dma((CHUNKS,)),
            dma,
            dma((CHUNKS,)),
            dma((2,)),
            dma((2,)),
            dma((GROUPS,)),
            dma,
            dma((BANDS,)),
            dma,
            dma,
            pltpu.SemaphoreType.REGULAR,
        ],
        compiler_params=pltpu.CompilerParams(
            collective_id=0, has_side_effects=True, vmem_limit_bytes=60 * 2**20),
    )(left_matrix, right_matrix)
    return own + copied


def gathered_product(left_matrix, right_matrix, layers):
    layer_index = lax.axis_index("layer")
    local_cols = right_matrix.shape[2]
    left_width = left_matrix.shape[2]
    right_height = right_matrix.shape[1]
    share_width = left_width // layers
    group_count = right_height // left_width
    left_own = lax.dynamic_slice_in_dim(left_matrix, layer_index * share_width, share_width, 2)
    right_view = right_matrix.reshape(2, group_count, layers, share_width, local_cols)
    right_own = lax.dynamic_slice_in_dim(right_view, layer_index, 1, 2)
    right_own = right_own.reshape(2, group_count * share_width, local_cols)
    right_whole = lax.all_gather(right_own, "row", axis=1, tiled=True)
    left_whole = lax.all_gather(left_own, "col", axis=2, tiled=True)
    dot = functools.partial(
        jnp.dot, precision=lax.Precision.HIGHEST, preferred_element_type=jnp.float32)
    first_term = dot(left_whole[0], right_whole[0])
    second_term = dot(left_whole[1], right_whole[1])
    third_term = dot(left_whole[0] + left_whole[1], right_whole[0] + right_whole[1])
    partial_product = jnp.stack([first_term - second_term, third_term - first_term - second_term])
    return lax.psum(partial_product, "layer")


def local(left_matrix, right_matrix):
    layers = lax.axis_size("layer")
    rows = lax.axis_size("row")
    cols = lax.axis_size("col")
    if layers == 2 and rows == cols == 4:
        return lent_product(left_matrix, right_matrix, layers, rows)
    return gathered_product(left_matrix, right_matrix, layers)


def solution(mesh):
    in_specs = (P(None, "row", "col"), P(None, "row", "col"))
    out_specs = P(None, "row", "col")
    return jax.shard_map(local, mesh=mesh, in_specs=in_specs, out_specs=out_specs, check_vma=False)
```

```python
import functools

import jax
import jax.numpy as jnp
from jax import lax
from jax.experimental import pallas as pl
from jax.experimental.pallas import tpu as pltpu
from jax.sharding import PartitionSpec as P

CHUNKS = 16
FINE = 2
GROUPS = 4
EXTRA = 2
FILL = 2
LAG = 1
BANDS = 8
MESH = pl.DeviceIdType.MESH


def kernel(rows, left, right, qout, qin, abuf, bbuf, xbuf, ebuf, acc, xacc, xout, xin, pout, pin,
           own_sem, bsend, rsend, brecv, bown, ysend, yrecv, xsend, xrecv, esem, csend, crecv,
           psend, precv, qsend, qrecv, turn):
    x = lax.axis_index("layer")
    z = lax.axis_index("row")
    col = lax.axis_index("col")
    y = col // 2
    c = col % 2
    height = left.shape[1]
    width = right.shape[2]
    share = abuf.shape[3]
    step = share // CHUNKS
    fine = step // FINE
    tall = height // GROUPS
    parts = CHUNKS // GROUPS
    wide = share // parts
    fill = FILL * step
    last = rows - 1
    tail = CHUNKS - 1
    kept = CHUNKS - EXTRA
    base = x * share
    parity = z % 2
    at_low, at_high = z == 0, z == last
    at_end = at_low | at_high
    lends = (at_low & (c == 1)) | (at_high & (c == 0))
    helps = ((z == 1) & (c == 1)) | ((z == last - 1) & (c == 0))
    inward = jnp.where(at_low, 1, last - 1)
    outward = jnp.where(z == 1, 0, last)
    far = jnp.where(z < rows // 2, last, 0)
    lent_slot = jnp.where(at_low, 0, (last - 1) // 2)
    lends_own = lends & (y == lent_slot)
    lends_relayed = lends & (y != lent_slot)

    def other(**where):
        return dict(device_id=where, device_id_type=MESH)

    partner = dict(col=y * 2 + 1 - c)
    across = dict(col=(1 - y) * 2 + c)
    copy_x = dict(layer=1 - x)

    barrier = pltpu.get_barrier_semaphore()
    for where in (partner, across, copy_x):
        pl.semaphore_signal(barrier, inc=1, **other(**where))

    @pl.when(z > 0)
    def _():
        for core in range(2):
            pl.semaphore_signal(barrier, inc=1, **other(row=z - 1, col=y * 2 + core))

    @pl.when(z < last)
    def _():
        for core in range(2):
            pl.semaphore_signal(barrier, inc=1, **other(row=z + 1, col=y * 2 + core))

    own_copy = pltpu.make_async_copy(left.at[:, :, pl.ds(base, share)], abuf.at[y], own_sem)
    own_copy.start()
    acc[...] = jnp.zeros_like(acc)
    xacc[...] = jnp.zeros_like(xacc)
    pl.semaphore_wait(barrier, 3 + 2 * ((z > 0).astype(jnp.int32) + (z < last).astype(jnp.int32)))

    def span(i):
        return pl.ds(pl.multiple_of(i * step, step), step)

    def source_span(i):
        return pl.ds(pl.multiple_of(base + i * step, step), step)

    def fine_span(u):
        return pl.ds(pl.multiple_of(u * fine, fine), fine)

    def fine_source(u):
        return pl.ds(pl.multiple_of(base + u * fine, fine), fine)

    def half(h):
        return pl.ds(pl.multiple_of(h * width, width), width)

    thin = height // BANDS
    per = BANDS // GROUPS

    def band_of(b):
        return pl.ds(pl.multiple_of(b * thin, thin), thin)

    def group(g):
        return pl.ds(pl.multiple_of(g * tall, tall), tall)

    def piece_rows(i):
        return group(i // parts)

    def piece_cols(i):
        return pl.ds(pl.multiple_of((i % parts) * wide, wide), wide)

    def piece_source(i):
        return pl.ds(pl.multiple_of(base + (i % parts) * wide, step), wide)

    whole_source = pl.ds(pl.multiple_of(base, step), share)

    def b_copy(u, way, row):
        return pltpu.make_async_remote_copy(
            src_ref=right.at[:, fine_source(u), :],
            dst_ref=bbuf.at[z // 2, c, :, fine_span(u), :],
            send_sem=bsend.at[way], recv_sem=brecv.at[z // 2, u],
            **other(row=row, col=y * 2 + parity))

    def b_sent(way):
        return pltpu.make_async_remote_copy(
            src_ref=right.at[:, whole_source, :], dst_ref=bbuf.at[z // 2, c],
            send_sem=bsend.at[way], recv_sem=bown.at[1], **other(**partner))

    b_local = pltpu.make_async_copy(right.at[:, whole_source, :], bbuf.at[z // 2, c], bown.at[0])
    b_partner = b_sent(2)

    def y_part(i):
        return (i == tail).astype(jnp.int32) if not isinstance(i, int) else int(i == tail)

    def y_copy(i):
        return pltpu.make_async_remote_copy(
            src_ref=left.at[:, :, source_span(i)], dst_ref=abuf.at[y, :, :, span(i)],
            send_sem=ysend.at[y_part(i)], recv_sem=yrecv.at[i], **other(**across))

    def y_piece(i):
        return pltpu.make_async_remote_copy(
            src_ref=left.at[:, piece_rows(i), piece_source(i)],
            dst_ref=abuf.at[y, :, piece_rows(i), piece_cols(i)],
            send_sem=ysend.at[y_part(i)], recv_sem=yrecv.at[i], **other(**across))

    def late(i):
        return i >= kept

    late_span = pl.ds(kept * step, EXTRA * step)
    late_source = pl.ds(pl.multiple_of(base + kept * step, step), EXTRA * step)

    def y_sent(part):
        size = (tail if part == 0 else 1) * step
        ref = abuf.at[y, :, :, pl.ds(0, size)]
        return pltpu.make_async_remote_copy(
            src_ref=ref, dst_ref=ref, send_sem=ysend.at[part], recv_sem=yrecv.at[0], **other(**across))

    def y_arrival(i):
        ref = abuf.at[1 - y, :, :, span(i)]
        return pltpu.make_async_copy(ref, ref, yrecv.at[i])

    def y_piece_arrival(i):
        ref = abuf.at[1 - y, :, piece_rows(i), piece_cols(i)]
        return pltpu.make_async_copy(ref, ref, yrecv.at[i])

    def by_piece(i, act):
        @pl.when(i % parts == 0)
        def _():
            act(piece_rows(i), fill, pl.multiple_of(base + fill, step), wide - fill)

        @pl.when(i % parts != 0)
        def _():
            start = pl.multiple_of((i % parts) * wide, wide)
            act(piece_rows(i), start, pl.multiple_of(base + start, step), wide)

    def x_own(i):
        def act(band, start, source, size):
            pltpu.make_async_remote_copy(
                src_ref=left.at[:, band, pl.ds(source, size)],
                dst_ref=xbuf.at[:, band, pl.ds(start, size)],
                send_sem=xsend, recv_sem=xrecv.at[i], **other(row=inward)).start()
        by_piece(i, act)

    def x_relay(i):
        def act(band, start, source, size):
            pltpu.make_async_remote_copy(
                src_ref=abuf.at[1 - y, :, band, pl.ds(start, size)],
                dst_ref=xbuf.at[:, band, pl.ds(start, size)],
                send_sem=xsend, recv_sem=xrecv.at[i], **other(row=inward)).start()
        by_piece(i, act)

    lent_ref = xbuf.at[:, :, pl.ds(fill, share - fill)]
    x_sent = pltpu.make_async_remote_copy(
        src_ref=lent_ref, dst_ref=lent_ref, send_sem=xsend, recv_sem=xrecv.at[0], **other(row=inward))
    e_own = pltpu.make_async_remote_copy(
        src_ref=left.at[:, :, late_source], dst_ref=ebuf,
        send_sem=esem.at[0], recv_sem=esem.at[1], **other(row=inward))
    e_relay = pltpu.make_async_remote_copy(
        src_ref=abuf.at[1 - y, :, :, late_span], dst_ref=ebuf,
        send_sem=esem.at[0], recv_sem=esem.at[1], **other(row=inward))

    yields = at_end & jnp.logical_not(lends) & (y == lent_slot)
    sends_up = (z < last) & (z != last - 1)
    sends_down = (z > 0) & (z != 1)

    fills_down = z == 1
    fills_up = z == last - 1
    fill_row = jnp.where(fills_down, 0, last)

    @pl.when(fills_down | fills_up)
    def _():
        for u in range(FILL * FINE):
            b_copy(u, 3, fill_row).start()

    @pl.when(lends_relayed)
    def _():
        for i in range(kept, CHUNKS):
            y_copy(i).start()

    def launch(i, carry):
        for k in range(FINE):
            @pl.when(sends_up)
            def _():
                b_copy(i * FINE + k, 0, z + 1).start()

            @pl.when(sends_down)
            def _():
                b_copy(i * FINE + k, 1, z - 1).start()

        @pl.when(jnp.logical_not(yields | lends_own) & jnp.logical_not(lends_relayed & late(i)))
        def _():
            y_copy(i).start()

        @pl.when(lends_own)
        def _():
            y_piece(i).start()

        return carry

    lax.fori_loop(0, CHUNKS, launch, 0)

    @pl.when(c == parity)
    def _():
        b_local.start()

    @pl.when(c != parity)
    def _():
        b_partner.start()

    @pl.when(lends_relayed)
    def _():
        e_own.start()

    @pl.when(lends_own)
    def _():
        for i in range(kept, CHUNKS):
            y_arrival(i).wait()
        e_relay.start()

        def lend(i, carry):
            x_own(i)
            return carry
        lax.fori_loop(0, CHUNKS, lend, 0)
        y_sent(0).wait_send()
        pl.semaphore_signal(turn, inc=1, **other(**partner))

    @pl.when(yields)
    def _():
        pl.semaphore_wait(turn, 1)

        def cross(i, carry):
            y_copy(i).start()
            return carry
        lax.fori_loop(0, CHUNKS, cross, 0)

    own_copy.wait()

    @pl.when(c == parity)
    def _():
        b_local.wait()
        b_sent(2).wait_recv()

    def b_arrival(s, u):
        ref = bbuf.at[s, :, :, fine_span(u), :]
        return pltpu.make_async_copy(ref, ref, brecv.at[s, u])

    def relay(s, u, part, row):
        ref = bbuf.at[s, :, :, fine_span(u), :]
        return pltpu.make_async_remote_copy(
            src_ref=ref, dst_ref=ref, send_sem=rsend.at[s, part], recv_sem=brecv.at[s, u],
            **other(row=row))

    def relayed(s, part):
        start, size = ((0, kept) if part == 0 else (kept, EXTRA))
        ref = bbuf.at[s, :, :, pl.ds(start * step, size * step), :]
        return pltpu.make_async_remote_copy(
            src_ref=ref, dst_ref=ref, send_sem=rsend.at[s, part], recv_sem=brecv.at[s, 0],
            **other(row=inward))

    def present(s):
        quarter = 2 * s + c
        return jnp.logical_not((at_low & (quarter == 1)) | (at_high & (quarter == last - 1)))

    def is_own(s):
        return 2 * s + c == z

    def is_far(s):
        return 2 * s + c == far

    def goes_up(s):
        quarter = 2 * s + c
        return (quarter < z) & (z < last)

    def goes_down(s):
        quarter = 2 * s + c
        return (quarter > z) & (z > 0)

    def goes(s, i):
        cut = is_far(s) & ((z == 1) | (z == last - 1)) & late(i)
        return (goes_up(s) | goes_down(s)) & jnp.logical_not(cut)

    def split(value):
        high = value.astype(jnp.bfloat16)
        return high, (value - high.astype(jnp.float32)).astype(jnp.bfloat16)

    def dot(a, b):
        a_high, a_low = split(a)
        b_high, b_low = split(b)
        return jnp.dot(
            jnp.concatenate([a_high, a_high, a_low], axis=1),
            jnp.concatenate([b_high, b_low, b_high], axis=0),
            preferred_element_type=jnp.float32)

    def both(s, at):
        return (jnp.concatenate([bbuf[s, h, k, at, :] for h in range(2)], axis=1) for k in range(2))

    def accumulate(a_ref, s, at):
        a_re, a_im = a_ref[0, :, at], a_ref[1, :, at]
        b_re, b_im = both(s, at)
        acc[0] += dot(a_re, b_re)
        acc[1] += dot(a_im, b_im)
        acc[2] += dot(a_re + a_im, b_re + b_im)

    def multiply(a_ref, s, i):

        @pl.when((i % 2 == 1) & jnp.logical_not(at_end & is_far(s) & late(i)))
        def _():
            accumulate(a_ref, s, pl.ds(pl.multiple_of((i - 1) * step, 2 * step), 2 * step))

    def lent_step(i):
        def act(band, start, source, size):
            ref = xbuf.at[:, band, pl.ds(start, size)]
            pltpu.make_async_copy(ref, ref, xrecv.at[i]).wait()
            at = pl.ds(start, size)
            a_re, a_im = xbuf[0, band, at], xbuf[1, band, at]
            b_re, b_im = both(z // 2, at)
            xacc[0, band] += dot(a_re, b_re)
            xacc[1, band] += dot(a_im, b_im)
            xacc[2, band] += dot(a_re + a_im, b_re + b_im)
        by_piece(i, act)

    def combined(totals, h, g):
        first, second, third = (totals[k, group(g), half(h)] for k in range(3))
        return first - second, third - first - second

    def lend_back(h, b):
        return pltpu.make_async_remote_copy(
            src_ref=xout.at[h, :, band_of(b)], dst_ref=xin.at[:, band_of(b)],
            send_sem=csend.at[h], recv_sem=crecv.at[b], **other(row=outward, col=y * 2 + h))

    def lent_back(h):
        return pltpu.make_async_remote_copy(
            src_ref=xout.at[h], dst_ref=xin, send_sem=csend.at[h], recv_sem=crecv.at[0],
            **other(row=outward, col=y * 2 + h))

    def lent_arrival(b):
        ref = xin.at[:, band_of(b)]
        return pltpu.make_async_copy(ref, ref, crecv.at[b])

    def give(g):
        for h in range(2):
            xout[h, 0, group(g)], xout[h, 1, group(g)] = combined(xacc, h, g)
        for k in range(per):
            for h in range(2):
                lend_back(h, g * per + k).start()

    def extra_step(i):
        @pl.when(i == kept)
        def _():
            e_own.wait_recv()

        b_re, b_im = both(1 - z // 2, span(i))
        b_sum = b_re + b_im
        at = span(i - kept)

        def add(g):
            band = group(g)
            a_re, a_im = ebuf[0, band, at], ebuf[1, band, at]
            xacc[0, band] += dot(a_re, b_re)
            xacc[1, band] += dot(a_im, b_im)
            xacc[2, band] += dot(a_re + a_im, b_sum)

        for g in range(GROUPS):
            add(g)
            if g < GROUPS - 1:
                @pl.when(i == tail)
                def _():
                    give(g)

    def right_step(i):
        for n in range(2):
            s = jnp.where(z < rows // 2, 1 - n, n)

            @pl.when(present(s) & jnp.logical_not(is_own(s)) & jnp.logical_not(at_end & is_far(s) & late(i)))
            def _():
                for k in range(FINE):
                    b_arrival(s, i * FINE + k).wait()

                    @pl.when(goes(s, i))
                    def _():
                        relay(s, i * FINE + k, late(i).astype(jnp.int32),
                              jnp.where(goes_up(s), z + 1, z - 1)).start()

        @pl.when(helps & late(i))
        def _():
            extra_step(i)

        @pl.when(lends & (i == 0))
        def _():
            for u in range(FILL * FINE):
                b_arrival(lent_slot, u).wait()
            accumulate(abuf.at[lent_slot], lent_slot, pl.ds(0, fill))

        @pl.when(present(y))
        def _():
            multiply(abuf.at[y], y, i)

    def left_step(i):
        @pl.when(jnp.logical_not(lends_relayed | (lends_own & late(i))))
        def _():
            y_arrival(i).wait()

        @pl.when(lends_relayed)
        def _():
            y_piece_arrival(i).wait()
            x_relay(i)

        @pl.when(present(1 - y))
        def _():
            multiply(abuf.at[1 - y], 1 - y, i)

        @pl.when(helps & (i >= LAG))
        def _():
            lent_step(i - LAG)

    early = jnp.logical_not(at_end) & (c != parity)

    def work(t, carry):
        first = t < CHUNKS
        apart = jnp.where(first, t, t - CHUNKS)
        i = jnp.where(early | lends_relayed, apart, t // 2)
        is_left = ((early & jnp.logical_not(first)) | (lends_relayed & first)
                   | (jnp.logical_not(early | lends_relayed) & (t % 2 == 1)))

        @pl.when(is_left)
        def _():
            left_step(i)

        @pl.when(jnp.logical_not(is_left))
        def _():
            right_step(i)

        return carry

    lax.fori_loop(0, 2 * CHUNKS, work, 0)

    def banded(h, b):
        first, second, third = (acc[k, band_of(b), half(h)] for k in range(3))
        return first - second, third - first - second

    def to_partner(b):
        return pltpu.make_async_remote_copy(
            src_ref=pout.at[:, band_of(b)], dst_ref=pin.at[:, band_of(b)],
            send_sem=psend, recv_sem=precv.at[b], **other(**partner))

    def to_copy(b):
        return pltpu.make_async_remote_copy(
            src_ref=qout.at[:, band_of(b)], dst_ref=qin.at[:, band_of(b)],
            send_sem=qsend, recv_sem=qrecv, **other(**copy_x))

    def hand(b, carry):
        pout[0, band_of(b)], pout[1, band_of(b)] = banded(1 - c, b)
        to_partner(b).start()
        return carry

    lax.fori_loop(0, BANDS, hand, 0)

    @pl.when(helps)
    def _():
        def lent_rest(i, carry):
            lent_step(i)
            return carry
        lax.fori_loop(CHUNKS - LAG, CHUNKS, lent_rest, 0)
        give(GROUPS - 1)

    def gather(b, carry):
        band = band_of(b)
        mine_re, mine_im = banded(c, b)
        to_partner(b).wait_recv()
        qout[0, band] = mine_re + pin[0, band]
        qout[1, band] = mine_im + pin[1, band]

        @pl.when(at_end)
        def _():
            lent_arrival(b).wait()
            qout[:, band] += xin[:, band]

        to_copy(b).start()
        return carry

    lax.fori_loop(0, BANDS, gather, 0)

    @pl.when(sends_up)
    def _():
        b_sent(0).wait_send()

    @pl.when(sends_down)
    def _():
        b_sent(1).wait_send()

    @pl.when(c != parity)
    def _():
        b_partner.wait_send()

    @pl.when(fills_down | fills_up)
    def _():
        ref = bbuf.at[z // 2, c, :, pl.ds(0, fill), :]
        pltpu.make_async_remote_copy(
            src_ref=ref, dst_ref=ref, send_sem=bsend.at[3], recv_sem=bown.at[1],
            **other(**partner)).wait_send()

    @pl.when(jnp.logical_not(lends_own))
    def _():
        y_sent(0).wait_send()

    y_sent(1).wait_send()

    @pl.when(lends)
    def _():
        x_sent.wait_send()
        e_own.wait_send()

    for s in range(2):
        for part in range(2):
            @pl.when(present(s) & goes(s, tail * part))
            def _():
                relayed(s, part).wait_send()

    @pl.when(helps)
    def _():
        for h in range(2):
            lent_back(h).wait_send()

    whole_part = pltpu.make_async_remote_copy(
        src_ref=pout, dst_ref=pin, send_sem=psend, recv_sem=precv.at[0], **other(**partner))
    whole_part.wait_send()

    whole_copy = pltpu.make_async_remote_copy(
        src_ref=qout, dst_ref=qin, send_sem=qsend, recv_sem=qrecv, **other(**copy_x))
    whole_copy.wait()


def lent_product(left_matrix, right_matrix, layers, rows):
    height = left_matrix.shape[1]
    width = right_matrix.shape[2]
    share = left_matrix.shape[2] // layers
    f32 = jnp.float32
    dma = pltpu.SemaphoreType.DMA
    block = (2, height, width)
    own, copied = pl.pallas_call(
        functools.partial(kernel, rows),
        out_shape=[pltpu.VMEM(block, f32)] * 2,
        in_specs=[pl.BlockSpec(memory_space=pl.ANY)] * 2,
        out_specs=[pl.BlockSpec(memory_space=pltpu.VMEM)] * 2,
        scratch_shapes=[
            pltpu.VMEM((2, 2, height, share), f32),
            pltpu.VMEM((2, 2, 2, share, width), f32),
            pltpu.VMEM((2, height, share), f32),
            pltpu.VMEM((2, height, EXTRA * share // CHUNKS), f32),
            pltpu.VMEM((3, height, 2 * width), f32),
            pltpu.VMEM((3, height, 2 * width), f32),
            pltpu.VMEM((2,) + block, f32),
            pltpu.VMEM(block, f32),
            pltpu.VMEM(block, f32),
            pltpu.VMEM(block, f32),
            dma,
            dma((4,)),
            dma((2, 2)),
            dma((2, CHUNKS * FINE)),
            dma((2,)),
            dma((2,)),
            dma((CHUNKS,)),
            dma,
            dma((CHUNKS,)),
            dma((2,)),
            dma((2,)),
            dma((BANDS,)),
            dma,
            dma((BANDS,)),
            dma,
            dma,
            pltpu.SemaphoreType.REGULAR,
        ],
        compiler_params=pltpu.CompilerParams(
            collective_id=0, has_side_effects=True, vmem_limit_bytes=60 * 2**20),
    )(left_matrix, right_matrix)
    return own + copied


def gathered_product(left_matrix, right_matrix, layers):
    layer_index = lax.axis_index("layer")
    local_cols = right_matrix.shape[2]
    left_width = left_matrix.shape[2]
    right_height = right_matrix.shape[1]
    share_width = left_width // layers
    group_count = right_height // left_width
    left_own = lax.dynamic_slice_in_dim(left_matrix, layer_index * share_width, share_width, 2)
    right_view = right_matrix.reshape(2, group_count, layers, share_width, local_cols)
    right_own = lax.dynamic_slice_in_dim(right_view, layer_index, 1, 2)
    right_own = right_own.reshape(2, group_count * share_width, local_cols)
    right_whole = lax.all_gather(right_own, "row", axis=1, tiled=True)
    left_whole = lax.all_gather(left_own, "col", axis=2, tiled=True)
    dot = functools.partial(
        jnp.dot, precision=lax.Precision.HIGHEST, preferred_element_type=jnp.float32)
    first_term = dot(left_whole[0], right_whole[0])
    second_term = dot(left_whole[1], right_whole[1])
    third_term = dot(left_whole[0] + left_whole[1], right_whole[0] + right_whole[1])
    partial_product = jnp.stack([first_term - second_term, third_term - first_term - second_term])
    return lax.psum(partial_product, "layer")


def local(left_matrix, right_matrix):
    layers = lax.axis_size("layer")
    rows = lax.axis_size("row")
    cols = lax.axis_size("col")
    if layers == 2 and rows == cols == 4:
        return lent_product(left_matrix, right_matrix, layers, rows)
    return gathered_product(left_matrix, right_matrix, layers)


def solution(mesh):
    in_specs = (P(None, "row", "col"), P(None, "row", "col"))
    out_specs = P(None, "row", "col")
    return jax.shard_map(local, mesh=mesh, in_specs=in_specs, out_specs=out_specs, check_vma=False)
```

```python
import functools

import jax
import jax.numpy as jnp
from jax import lax
from jax.experimental import pallas as pl
from jax.experimental.pallas import tpu as pltpu
from jax.sharding import PartitionSpec as P

CHUNKS = 16
FINE = 2
GROUPS = 4
EXTRA = 2
FILL = 2
LAG = 1
BANDS = 8
MESH = pl.DeviceIdType.MESH


def kernel(rows, left, right, qout, qin, abuf, bbuf, xbuf, ebuf, acc, xacc, xout, xin, pout, pin,
           own_sem, bsend, rsend, brecv, bown, ysend, yrecv, xsend, xrecv, esem, csend, crecv,
           psend, precv, qsend, qrecv, turn):
    x = lax.axis_index("layer")
    z = lax.axis_index("row")
    col = lax.axis_index("col")
    y = col // 2
    c = col % 2
    height = left.shape[1]
    width = right.shape[2]
    share = abuf.shape[3]
    step = share // CHUNKS
    fine = step // FINE
    tall = height // GROUPS
    parts = CHUNKS // GROUPS
    wide = share // parts
    fill = FILL * step
    last = rows - 1
    tail = CHUNKS - 1
    kept = CHUNKS - EXTRA
    base = x * share
    parity = z % 2
    at_low, at_high = z == 0, z == last
    at_end = at_low | at_high
    lends = (at_low & (c == 1)) | (at_high & (c == 0))
    helps = ((z == 1) & (c == 1)) | ((z == last - 1) & (c == 0))
    inward = jnp.where(at_low, 1, last - 1)
    outward = jnp.where(z == 1, 0, last)
    far = jnp.where(z < rows // 2, last, 0)
    lent_slot = jnp.where(at_low, 0, (last - 1) // 2)
    lends_own = lends & (y == lent_slot)
    lends_relayed = lends & (y != lent_slot)

    def other(**where):
        return dict(device_id=where, device_id_type=MESH)

    partner = dict(col=y * 2 + 1 - c)
    across = dict(col=(1 - y) * 2 + c)
    copy_x = dict(layer=1 - x)

    barrier = pltpu.get_barrier_semaphore()
    for where in (partner, across, copy_x):
        pl.semaphore_signal(barrier, inc=1, **other(**where))

    @pl.when(z > 0)
    def _():
        for core in range(2):
            pl.semaphore_signal(barrier, inc=1, **other(row=z - 1, col=y * 2 + core))

    @pl.when(z < last)
    def _():
        for core in range(2):
            pl.semaphore_signal(barrier, inc=1, **other(row=z + 1, col=y * 2 + core))

    own_copy = pltpu.make_async_copy(left.at[:, :, pl.ds(base, share)], abuf.at[y], own_sem)
    own_copy.start()
    acc[...] = jnp.zeros_like(acc)
    xacc[...] = jnp.zeros_like(xacc)
    pl.semaphore_wait(barrier, 3 + 2 * ((z > 0).astype(jnp.int32) + (z < last).astype(jnp.int32)))

    def span(i):
        return pl.ds(pl.multiple_of(i * step, step), step)

    def source_span(i):
        return pl.ds(pl.multiple_of(base + i * step, step), step)

    def fine_span(u):
        return pl.ds(pl.multiple_of(u * fine, fine), fine)

    def fine_source(u):
        return pl.ds(pl.multiple_of(base + u * fine, fine), fine)

    def half(h):
        return pl.ds(pl.multiple_of(h * width, width), width)

    thin = height // BANDS
    per = BANDS // GROUPS

    def band_of(b):
        return pl.ds(pl.multiple_of(b * thin, thin), thin)

    def group(g):
        return pl.ds(pl.multiple_of(g * tall, tall), tall)

    def piece_rows(i):
        return group(i // parts)

    def piece_cols(i):
        return pl.ds(pl.multiple_of((i % parts) * wide, wide), wide)

    def piece_source(i):
        return pl.ds(pl.multiple_of(base + (i % parts) * wide, step), wide)

    whole_source = pl.ds(pl.multiple_of(base, step), share)

    def b_copy(u, way, row):
        return pltpu.make_async_remote_copy(
            src_ref=right.at[:, fine_source(u), :],
            dst_ref=bbuf.at[z // 2, c, :, fine_span(u), :],
            send_sem=bsend.at[way], recv_sem=brecv.at[z // 2, u],
            **other(row=row, col=y * 2 + parity))

    def b_sent(way):
        return pltpu.make_async_remote_copy(
            src_ref=right.at[:, whole_source, :], dst_ref=bbuf.at[z // 2, c],
            send_sem=bsend.at[way], recv_sem=bown.at[1], **other(**partner))

    b_local = pltpu.make_async_copy(right.at[:, whole_source, :], bbuf.at[z // 2, c], bown.at[0])
    b_partner = b_sent(2)

    def y_part(i):
        return (i == tail).astype(jnp.int32) if not isinstance(i, int) else int(i == tail)

    def y_copy(i):
        return pltpu.make_async_remote_copy(
            src_ref=left.at[:, :, source_span(i)], dst_ref=abuf.at[y, :, :, span(i)],
            send_sem=ysend.at[y_part(i)], recv_sem=yrecv.at[i], **other(**across))

    def y_piece(i):
        return pltpu.make_async_remote_copy(
            src_ref=left.at[:, piece_rows(i), piece_source(i)],
            dst_ref=abuf.at[y, :, piece_rows(i), piece_cols(i)],
            send_sem=ysend.at[y_part(i)], recv_sem=yrecv.at[i], **other(**across))

    def late(i):
        return i >= kept

    late_span = pl.ds(kept * step, EXTRA * step)
    late_source = pl.ds(pl.multiple_of(base + kept * step, step), EXTRA * step)

    def y_sent(part):
        size = (tail if part == 0 else 1) * step
        ref = abuf.at[y, :, :, pl.ds(0, size)]
        return pltpu.make_async_remote_copy(
            src_ref=ref, dst_ref=ref, send_sem=ysend.at[part], recv_sem=yrecv.at[0], **other(**across))

    def y_arrival(i):
        ref = abuf.at[1 - y, :, :, span(i)]
        return pltpu.make_async_copy(ref, ref, yrecv.at[i])

    def y_piece_arrival(i):
        ref = abuf.at[1 - y, :, piece_rows(i), piece_cols(i)]
        return pltpu.make_async_copy(ref, ref, yrecv.at[i])

    def by_piece(i, act):
        @pl.when(i % parts == 0)
        def _():
            act(piece_rows(i), fill, pl.multiple_of(base + fill, step), wide - fill)

        @pl.when(i % parts != 0)
        def _():
            start = pl.multiple_of((i % parts) * wide, wide)
            act(piece_rows(i), start, pl.multiple_of(base + start, step), wide)

    def x_own(i):
        def act(band, start, source, size):
            pltpu.make_async_remote_copy(
                src_ref=left.at[:, band, pl.ds(source, size)],
                dst_ref=xbuf.at[:, band, pl.ds(start, size)],
                send_sem=xsend, recv_sem=xrecv.at[i], **other(row=inward)).start()
        by_piece(i, act)

    def x_relay(i):
        def act(band, start, source, size):
            pltpu.make_async_remote_copy(
                src_ref=abuf.at[1 - y, :, band, pl.ds(start, size)],
                dst_ref=xbuf.at[:, band, pl.ds(start, size)],
                send_sem=xsend, recv_sem=xrecv.at[i], **other(row=inward)).start()
        by_piece(i, act)

    lent_ref = xbuf.at[:, :, pl.ds(fill, share - fill)]
    x_sent = pltpu.make_async_remote_copy(
        src_ref=lent_ref, dst_ref=lent_ref, send_sem=xsend, recv_sem=xrecv.at[0], **other(row=inward))
    e_own = pltpu.make_async_remote_copy(
        src_ref=left.at[:, :, late_source], dst_ref=ebuf,
        send_sem=esem.at[0], recv_sem=esem.at[1], **other(row=inward))
    e_relay = pltpu.make_async_remote_copy(
        src_ref=abuf.at[1 - y, :, :, late_span], dst_ref=ebuf,
        send_sem=esem.at[0], recv_sem=esem.at[1], **other(row=inward))

    yields = at_end & jnp.logical_not(lends) & (y == lent_slot)
    sends_up = (z < last) & (z != last - 1)
    sends_down = (z > 0) & (z != 1)

    fills_down = z == 1
    fills_up = z == last - 1
    fill_row = jnp.where(fills_down, 0, last)

    @pl.when(fills_down | fills_up)
    def _():
        for u in range(FILL * FINE):
            b_copy(u, 3, fill_row).start()

    @pl.when(lends_relayed)
    def _():
        for i in range(kept, CHUNKS):
            y_copy(i).start()

    def launch(i, carry):
        for k in range(FINE):
            @pl.when(sends_up)
            def _():
                b_copy(i * FINE + k, 0, z + 1).start()

            @pl.when(sends_down)
            def _():
                b_copy(i * FINE + k, 1, z - 1).start()

        @pl.when(jnp.logical_not(yields | lends_own) & jnp.logical_not(lends_relayed & late(i)))
        def _():
            y_copy(i).start()

        @pl.when(lends_own)
        def _():
            y_piece(i).start()

        return carry

    lax.fori_loop(0, CHUNKS, launch, 0)

    @pl.when(c == parity)
    def _():
        b_local.start()

    @pl.when(c != parity)
    def _():
        b_partner.start()

    @pl.when(lends_relayed)
    def _():
        e_own.start()

    @pl.when(lends_own)
    def _():
        for i in range(kept, CHUNKS):
            y_arrival(i).wait()
        e_relay.start()

        def lend(i, carry):
            x_own(i)
            return carry
        lax.fori_loop(0, CHUNKS, lend, 0)
        y_sent(0).wait_send()
        pl.semaphore_signal(turn, inc=1, **other(**partner))

    @pl.when(yields)
    def _():
        pl.semaphore_wait(turn, 1)

        def cross(i, carry):
            y_copy(i).start()
            return carry
        lax.fori_loop(0, CHUNKS, cross, 0)

    own_copy.wait()

    @pl.when(c == parity)
    def _():
        b_local.wait()
        b_sent(2).wait_recv()

    def b_arrival(s, u):
        ref = bbuf.at[s, :, :, fine_span(u), :]
        return pltpu.make_async_copy(ref, ref, brecv.at[s, u])

    def relay(s, u, part, row):
        ref = bbuf.at[s, :, :, fine_span(u), :]
        return pltpu.make_async_remote_copy(
            src_ref=ref, dst_ref=ref, send_sem=rsend.at[s, part], recv_sem=brecv.at[s, u],
            **other(row=row))

    def half_relay(s, h, row):
        ref = bbuf.at[s, h, :, late_span, :]
        return pltpu.make_async_remote_copy(
            src_ref=ref, dst_ref=ref, send_sem=rsend.at[s, 1],
            recv_sem=brecv.at[s, kept * FINE + h], **other(row=row))

    def relayed(s, part):
        start, size = ((0, kept) if part == 0 else (kept, EXTRA))
        ref = bbuf.at[s, :, :, pl.ds(start * step, size * step), :]
        return pltpu.make_async_remote_copy(
            src_ref=ref, dst_ref=ref, send_sem=rsend.at[s, part], recv_sem=brecv.at[s, 0],
            **other(row=inward))

    def present(s):
        quarter = 2 * s + c
        return jnp.logical_not((at_low & (quarter == 1)) | (at_high & (quarter == last - 1)))

    def is_own(s):
        return 2 * s + c == z

    def is_outer(s):
        outer = jnp.where(z < rows // 2, 0, last)
        return (2 * s + c == outer) & jnp.logical_not(at_end)

    def is_far(s):
        return 2 * s + c == far

    def goes_up(s):
        quarter = 2 * s + c
        return (quarter < z) & (z < last)

    def goes_down(s):
        quarter = 2 * s + c
        return (quarter > z) & (z > 0)

    def goes(s, i):
        cut = is_far(s) & ((z == 1) | (z == last - 1)) & late(i)
        return (goes_up(s) | goes_down(s)) & jnp.logical_not(cut)

    def split(value):
        high = value.astype(jnp.bfloat16)
        return high, (value - high.astype(jnp.float32)).astype(jnp.bfloat16)

    def dot(a, b):
        a_high, a_low = split(a)
        b_high, b_low = split(b)
        return jnp.dot(
            jnp.concatenate([a_high, a_high, a_low], axis=1),
            jnp.concatenate([b_high, b_low, b_high], axis=0),
            preferred_element_type=jnp.float32)

    def both(s, at):
        return (jnp.concatenate([bbuf[s, h, k, at, :] for h in range(2)], axis=1) for k in range(2))

    def accumulate(a_ref, s, at):
        a_re, a_im = a_ref[0, :, at], a_ref[1, :, at]
        b_re, b_im = both(s, at)
        acc[0] += dot(a_re, b_re)
        acc[1] += dot(a_im, b_im)
        acc[2] += dot(a_re + a_im, b_re + b_im)

    def multiply(a_ref, s, i):

        @pl.when((i % 2 == 1) & jnp.logical_not(at_end & is_far(s) & late(i)))
        def _():
            accumulate(a_ref, s, pl.ds(pl.multiple_of((i - 1) * step, 2 * step), 2 * step))

    def lent_step(i):
        def act(band, start, source, size):
            ref = xbuf.at[:, band, pl.ds(start, size)]
            pltpu.make_async_copy(ref, ref, xrecv.at[i]).wait()
            at = pl.ds(start, size)
            a_re, a_im = xbuf[0, band, at], xbuf[1, band, at]
            b_re, b_im = both(z // 2, at)
            xacc[0, band] += dot(a_re, b_re)
            xacc[1, band] += dot(a_im, b_im)
            xacc[2, band] += dot(a_re + a_im, b_re + b_im)
        by_piece(i, act)

    def combined(totals, h, g):
        first, second, third = (totals[k, group(g), half(h)] for k in range(3))
        return first - second, third - first - second

    def lend_back(h, b):
        return pltpu.make_async_remote_copy(
            src_ref=xout.at[h, :, band_of(b)], dst_ref=xin.at[:, band_of(b)],
            send_sem=csend.at[h], recv_sem=crecv.at[b], **other(row=outward, col=y * 2 + h))

    def lent_back(h):
        return pltpu.make_async_remote_copy(
            src_ref=xout.at[h], dst_ref=xin, send_sem=csend.at[h], recv_sem=crecv.at[0],
            **other(row=outward, col=y * 2 + h))

    def lent_arrival(b):
        ref = xin.at[:, band_of(b)]
        return pltpu.make_async_copy(ref, ref, crecv.at[b])

    def give(h, g):
        xout[h, 0, group(g)], xout[h, 1, group(g)] = combined(xacc, h, g)
        for k in range(per):
            lend_back(h, g * per + k).start()

    def extra_step(h):
        if h == 0:
            e_own.wait_recv()

        b_re, b_im = (bbuf[1 - z // 2, h, k, late_span, :] for k in range(2))
        b_sum = b_re + b_im
        lanes = half(h)

        for g in range(GROUPS):
            band = group(g)
            a_re, a_im = ebuf[0, band, :], ebuf[1, band, :]
            xacc[0, band, lanes] += dot(a_re, b_re)
            xacc[1, band, lanes] += dot(a_im, b_im)
            xacc[2, band, lanes] += dot(a_re + a_im, b_sum)
            if h == 1 or g < GROUPS - 1:
                give(h, g)

    def right_step(i):
        @pl.when(helps & (i == tail))
        def _():
            for k in range(LAG + 1):
                lent_step(i - LAG + k)
            give(0, GROUPS - 1)

        for n in range(2):
            s = jnp.where(z < rows // 2, 1 - n, n)

            @pl.when(present(s) & jnp.logical_not(is_own(s)) & jnp.logical_not(at_end & is_far(s) & late(i)))
            def _():
                onward = jnp.where(goes_up(s), z + 1, z - 1)
                in_halves = late(i) & helps & is_far(s)
                by_halves = late(i) & is_outer(s)

                @pl.when(jnp.logical_not(in_halves))
                def _():
                    for k in range(FINE):
                        b_arrival(s, i * FINE + k).wait()

                        @pl.when(goes(s, i) & jnp.logical_not(by_halves))
                        def _():
                            relay(s, i * FINE + k, late(i).astype(jnp.int32), onward).start()

                @pl.when(by_halves & (i == tail))
                def _():
                    for h in range(2):
                        half_relay(s, h, onward).start()

                @pl.when(in_halves)
                def _():
                    ref = bbuf.at[s, i - kept, :, late_span, :]
                    pltpu.make_async_copy(ref, ref, brecv.at[s, kept * FINE + i - kept]).wait()

        @pl.when(helps & (i == kept))
        def _():
            extra_step(0)

        @pl.when(lends & (i == 0))
        def _():
            for u in range(FILL * FINE):
                b_arrival(lent_slot, u).wait()
            accumulate(abuf.at[lent_slot], lent_slot, pl.ds(0, fill))

        @pl.when(present(y))
        def _():
            multiply(abuf.at[y], y, i)

    def left_step(i):
        @pl.when(jnp.logical_not(lends_relayed | (lends_own & late(i))))
        def _():
            y_arrival(i).wait()

        @pl.when(lends_relayed)
        def _():
            y_piece_arrival(i).wait()
            x_relay(i)

        @pl.when(present(1 - y))
        def _():
            multiply(abuf.at[1 - y], 1 - y, i)

        @pl.when(helps & (i >= LAG) & (i < tail))
        def _():
            lent_step(i - LAG)

    early = jnp.logical_not(at_end) & (c != parity)

    def work(t, carry):
        first = t < CHUNKS
        apart = jnp.where(first, t, t - CHUNKS)
        i = jnp.where(early | lends_relayed, apart, t // 2)
        is_left = ((early & jnp.logical_not(first)) | (lends_relayed & first)
                   | (jnp.logical_not(early | lends_relayed) & (t % 2 == 1)))

        @pl.when(is_left)
        def _():
            left_step(i)

        @pl.when(jnp.logical_not(is_left))
        def _():
            right_step(i)

        return carry

    lax.fori_loop(0, 2 * CHUNKS, work, 0)

    def banded(h, b):
        first, second, third = (acc[k, band_of(b), half(h)] for k in range(3))
        return first - second, third - first - second

    def to_partner(b):
        return pltpu.make_async_remote_copy(
            src_ref=pout.at[:, band_of(b)], dst_ref=pin.at[:, band_of(b)],
            send_sem=psend, recv_sem=precv.at[b], **other(**partner))

    def to_copy(b):
        return pltpu.make_async_remote_copy(
            src_ref=qout.at[:, band_of(b)], dst_ref=qin.at[:, band_of(b)],
            send_sem=qsend, recv_sem=qrecv, **other(**copy_x))

    def hand(b, carry):
        pout[0, band_of(b)], pout[1, band_of(b)] = banded(1 - c, b)
        to_partner(b).start()
        return carry

    lax.fori_loop(0, BANDS, hand, 0)

    @pl.when(helps)
    def _():
        extra_step(1)

    def gather(b, carry):
        band = band_of(b)
        mine_re, mine_im = banded(c, b)
        to_partner(b).wait_recv()
        qout[0, band] = mine_re + pin[0, band]
        qout[1, band] = mine_im + pin[1, band]

        @pl.when(at_end)
        def _():
            lent_arrival(b).wait()
            qout[:, band] += xin[:, band]

        to_copy(b).start()
        return carry

    lax.fori_loop(0, BANDS, gather, 0)

    @pl.when(sends_up)
    def _():
        b_sent(0).wait_send()

    @pl.when(sends_down)
    def _():
        b_sent(1).wait_send()

    @pl.when(c != parity)
    def _():
        b_partner.wait_send()

    @pl.when(fills_down | fills_up)
    def _():
        ref = bbuf.at[z // 2, c, :, pl.ds(0, fill), :]
        pltpu.make_async_remote_copy(
            src_ref=ref, dst_ref=ref, send_sem=bsend.at[3], recv_sem=bown.at[1],
            **other(**partner)).wait_send()

    @pl.when(jnp.logical_not(lends_own))
    def _():
        y_sent(0).wait_send()

    y_sent(1).wait_send()

    @pl.when(lends)
    def _():
        x_sent.wait_send()
        e_own.wait_send()

    for s in range(2):
        for part in range(2):
            @pl.when(present(s) & goes(s, tail * part))
            def _():
                relayed(s, part).wait_send()

    @pl.when(helps)
    def _():
        for h in range(2):
            lent_back(h).wait_send()

    whole_part = pltpu.make_async_remote_copy(
        src_ref=pout, dst_ref=pin, send_sem=psend, recv_sem=precv.at[0], **other(**partner))
    whole_part.wait_send()

    whole_copy = pltpu.make_async_remote_copy(
        src_ref=qout, dst_ref=qin, send_sem=qsend, recv_sem=qrecv, **other(**copy_x))
    whole_copy.wait()


def lent_product(left_matrix, right_matrix, layers, rows):
    height = left_matrix.shape[1]
    width = right_matrix.shape[2]
    share = left_matrix.shape[2] // layers
    f32 = jnp.float32
    dma = pltpu.SemaphoreType.DMA
    block = (2, height, width)
    own, copied = pl.pallas_call(
        functools.partial(kernel, rows),
        out_shape=[pltpu.VMEM(block, f32)] * 2,
        in_specs=[pl.BlockSpec(memory_space=pl.ANY)] * 2,
        out_specs=[pl.BlockSpec(memory_space=pltpu.VMEM)] * 2,
        scratch_shapes=[
            pltpu.VMEM((2, 2, height, share), f32),
            pltpu.VMEM((2, 2, 2, share, width), f32),
            pltpu.VMEM((2, height, share), f32),
            pltpu.VMEM((2, height, EXTRA * share // CHUNKS), f32),
            pltpu.VMEM((3, height, 2 * width), f32),
            pltpu.VMEM((3, height, 2 * width), f32),
            pltpu.VMEM((2,) + block, f32),
            pltpu.VMEM(block, f32),
            pltpu.VMEM(block, f32),
            pltpu.VMEM(block, f32),
            dma,
            dma((4,)),
            dma((2, 2)),
            dma((2, CHUNKS * FINE)),
            dma((2,)),
            dma((2,)),
            dma((CHUNKS,)),
            dma,
            dma((CHUNKS,)),
            dma((2,)),
            dma((2,)),
            dma((BANDS,)),
            dma,
            dma((BANDS,)),
            dma,
            dma,
            pltpu.SemaphoreType.REGULAR,
        ],
        compiler_params=pltpu.CompilerParams(
            collective_id=0, has_side_effects=True, vmem_limit_bytes=60 * 2**20),
    )(left_matrix, right_matrix)
    return own + copied


def gathered_product(left_matrix, right_matrix, layers):
    layer_index = lax.axis_index("layer")
    local_cols = right_matrix.shape[2]
    left_width = left_matrix.shape[2]
    right_height = right_matrix.shape[1]
    share_width = left_width // layers
    group_count = right_height // left_width
    left_own = lax.dynamic_slice_in_dim(left_matrix, layer_index * share_width, share_width, 2)
    right_view = right_matrix.reshape(2, group_count, layers, share_width, local_cols)
    right_own = lax.dynamic_slice_in_dim(right_view, layer_index, 1, 2)
    right_own = right_own.reshape(2, group_count * share_width, local_cols)
    right_whole = lax.all_gather(right_own, "row", axis=1, tiled=True)
    left_whole = lax.all_gather(left_own, "col", axis=2, tiled=True)
    dot = functools.partial(
        jnp.dot, precision=lax.Precision.HIGHEST, preferred_element_type=jnp.float32)
    first_term = dot(left_whole[0], right_whole[0])
    second_term = dot(left_whole[1], right_whole[1])
    third_term = dot(left_whole[0] + left_whole[1], right_whole[0] + right_whole[1])
    partial_product = jnp.stack([first_term - second_term, third_term - first_term - second_term])
    return lax.psum(partial_product, "layer")


def local(left_matrix, right_matrix):
    layers = lax.axis_size("layer")
    rows = lax.axis_size("row")
    cols = lax.axis_size("col")
    if layers == 2 and rows == cols == 4:
        return lent_product(left_matrix, right_matrix, layers, rows)
    return gathered_product(left_matrix, right_matrix, layers)


def solution(mesh):
    in_specs = (P(None, "row", "col"), P(None, "row", "col"))
    out_specs = P(None, "row", "col")
    return jax.shard_map(local, mesh=mesh, in_specs=in_specs, out_specs=out_specs, check_vma=False)
```

```python
import functools

import jax
import jax.numpy as jnp
from jax import lax
from jax.experimental import pallas as pl
from jax.experimental.pallas import tpu as pltpu
from jax.sharding import PartitionSpec as P

CHUNKS = 16
FINE = 2
GROUPS = 4
EXTRA = 2
FILL = 2
LAG = 1
BANDS = 8
MESH = pl.DeviceIdType.MESH


def kernel(rows, left, right, qout, qin, abuf, bbuf, xbuf, ebuf, acc, xacc, xout, xin, pout, pin,
           own_sem, bsend, rsend, brecv, bown, ysend, yrecv, xsend, xrecv, esem, csend, crecv,
           psend, precv, qsend, qrecv, turn):
    x = lax.axis_index("layer")
    z = lax.axis_index("row")
    col = lax.axis_index("col")
    y = col // 2
    c = col % 2
    height = left.shape[1]
    width = right.shape[2]
    share = abuf.shape[3]
    step = share // CHUNKS
    fine = step // FINE
    tall = height // GROUPS
    parts = CHUNKS // GROUPS
    wide = share // parts
    fill = FILL * step
    last = rows - 1
    tail = CHUNKS - 1
    kept = CHUNKS - EXTRA
    base = x * share
    parity = z % 2
    at_low, at_high = z == 0, z == last
    at_end = at_low | at_high
    lends = (at_low & (c == 1)) | (at_high & (c == 0))
    helps = ((z == 1) & (c == 1)) | ((z == last - 1) & (c == 0))
    inward = jnp.where(at_low, 1, last - 1)
    outward = jnp.where(z == 1, 0, last)
    far = jnp.where(z < rows // 2, last, 0)
    lent_slot = jnp.where(at_low, 0, (last - 1) // 2)
    lends_own = lends & (y == lent_slot)
    lends_relayed = lends & (y != lent_slot)

    def other(**where):
        return dict(device_id=where, device_id_type=MESH)

    partner = dict(col=y * 2 + 1 - c)
    across = dict(col=(1 - y) * 2 + c)
    copy_x = dict(layer=1 - x)

    barrier = pltpu.get_barrier_semaphore()
    for where in (partner, across, copy_x):
        pl.semaphore_signal(barrier, inc=1, **other(**where))

    @pl.when(z > 0)
    def _():
        for core in range(2):
            pl.semaphore_signal(barrier, inc=1, **other(row=z - 1, col=y * 2 + core))

    @pl.when(z < last)
    def _():
        for core in range(2):
            pl.semaphore_signal(barrier, inc=1, **other(row=z + 1, col=y * 2 + core))

    own_copy = pltpu.make_async_copy(left.at[:, :, pl.ds(base, share)], abuf.at[y], own_sem)
    own_copy.start()
    acc[...] = jnp.zeros_like(acc)
    xacc[...] = jnp.zeros_like(xacc)
    pl.semaphore_wait(barrier, 3 + 2 * ((z > 0).astype(jnp.int32) + (z < last).astype(jnp.int32)))

    def span(i):
        return pl.ds(pl.multiple_of(i * step, step), step)

    def source_span(i):
        return pl.ds(pl.multiple_of(base + i * step, step), step)

    def fine_span(u):
        return pl.ds(pl.multiple_of(u * fine, fine), fine)

    def fine_source(u):
        return pl.ds(pl.multiple_of(base + u * fine, fine), fine)

    def half(h):
        return pl.ds(pl.multiple_of(h * width, width), width)

    thin = height // BANDS
    per = BANDS // GROUPS

    def band_of(b):
        return pl.ds(pl.multiple_of(b * thin, thin), thin)

    def group(g):
        return pl.ds(pl.multiple_of(g * tall, tall), tall)

    def piece_rows(i):
        return group(i // parts)

    def piece_cols(i):
        return pl.ds(pl.multiple_of((i % parts) * wide, wide), wide)

    def piece_source(i):
        return pl.ds(pl.multiple_of(base + (i % parts) * wide, step), wide)

    whole_source = pl.ds(pl.multiple_of(base, step), share)

    def b_copy(u, way, row):
        return pltpu.make_async_remote_copy(
            src_ref=right.at[:, fine_source(u), :],
            dst_ref=bbuf.at[z // 2, c, :, fine_span(u), :],
            send_sem=bsend.at[way], recv_sem=brecv.at[z // 2, u],
            **other(row=row, col=y * 2 + parity))

    def b_sent(way):
        return pltpu.make_async_remote_copy(
            src_ref=right.at[:, whole_source, :], dst_ref=bbuf.at[z // 2, c],
            send_sem=bsend.at[way], recv_sem=bown.at[1], **other(**partner))

    b_local = pltpu.make_async_copy(right.at[:, whole_source, :], bbuf.at[z // 2, c], bown.at[0])
    b_partner = b_sent(2)

    def y_part(i):
        return (i == tail).astype(jnp.int32) if not isinstance(i, int) else int(i == tail)

    def y_copy(i):
        return pltpu.make_async_remote_copy(
            src_ref=left.at[:, :, source_span(i)], dst_ref=abuf.at[y, :, :, span(i)],
            send_sem=ysend.at[y_part(i)], recv_sem=yrecv.at[i], **other(**across))

    def y_piece(i):
        return pltpu.make_async_remote_copy(
            src_ref=left.at[:, piece_rows(i), piece_source(i)],
            dst_ref=abuf.at[y, :, piece_rows(i), piece_cols(i)],
            send_sem=ysend.at[y_part(i)], recv_sem=yrecv.at[i], **other(**across))

    def late(i):
        return i >= kept

    late_span = pl.ds(kept * step, EXTRA * step)
    late_source = pl.ds(pl.multiple_of(base + kept * step, step), EXTRA * step)

    def y_sent(part):
        size = (tail if part == 0 else 1) * step
        ref = abuf.at[y, :, :, pl.ds(0, size)]
        return pltpu.make_async_remote_copy(
            src_ref=ref, dst_ref=ref, send_sem=ysend.at[part], recv_sem=yrecv.at[0], **other(**across))

    def y_arrival(i):
        ref = abuf.at[1 - y, :, :, span(i)]
        return pltpu.make_async_copy(ref, ref, yrecv.at[i])

    def y_piece_arrival(i):
        ref = abuf.at[1 - y, :, piece_rows(i), piece_cols(i)]
        return pltpu.make_async_copy(ref, ref, yrecv.at[i])

    def by_piece(i, act):
        @pl.when(i % parts == 0)
        def _():
            act(piece_rows(i), fill, pl.multiple_of(base + fill, step), wide - fill)

        @pl.when(i % parts != 0)
        def _():
            start = pl.multiple_of((i % parts) * wide, wide)
            act(piece_rows(i), start, pl.multiple_of(base + start, step), wide)

    def x_own(i):
        def act(band, start, source, size):
            pltpu.make_async_remote_copy(
                src_ref=left.at[:, band, pl.ds(source, size)],
                dst_ref=xbuf.at[:, band, pl.ds(start, size)],
                send_sem=xsend, recv_sem=xrecv.at[i], **other(row=inward)).start()
        by_piece(i, act)

    def x_relay(i):
        def act(band, start, source, size):
            pltpu.make_async_remote_copy(
                src_ref=abuf.at[1 - y, :, band, pl.ds(start, size)],
                dst_ref=xbuf.at[:, band, pl.ds(start, size)],
                send_sem=xsend, recv_sem=xrecv.at[i], **other(row=inward)).start()
        by_piece(i, act)

    lent_ref = xbuf.at[:, :, pl.ds(fill, share - fill)]
    x_sent = pltpu.make_async_remote_copy(
        src_ref=lent_ref, dst_ref=lent_ref, send_sem=xsend, recv_sem=xrecv.at[0], **other(row=inward))
    e_own = pltpu.make_async_remote_copy(
        src_ref=left.at[:, :, late_source], dst_ref=ebuf,
        send_sem=esem.at[0], recv_sem=esem.at[1], **other(row=inward))
    e_relay = pltpu.make_async_remote_copy(
        src_ref=abuf.at[1 - y, :, :, late_span], dst_ref=ebuf,
        send_sem=esem.at[0], recv_sem=esem.at[1], **other(row=inward))

    defers = jnp.logical_not(at_end | helps)
    yields = at_end & jnp.logical_not(lends) & (y == lent_slot)
    sends_up = (z < last) & (z != last - 1)
    sends_down = (z > 0) & (z != 1)

    fills_down = z == 1
    fills_up = z == last - 1
    fill_row = jnp.where(fills_down, 0, last)

    @pl.when(fills_down | fills_up)
    def _():
        for u in range(FILL * FINE):
            b_copy(u, 3, fill_row).start()

    @pl.when(lends_relayed)
    def _():
        for i in range(kept, CHUNKS):
            y_copy(i).start()

    def launch(i, carry):
        for k in range(FINE):
            @pl.when(sends_up)
            def _():
                b_copy(i * FINE + k, 0, z + 1).start()

            @pl.when(sends_down)
            def _():
                b_copy(i * FINE + k, 1, z - 1).start()

        @pl.when(jnp.logical_not(yields | lends_own | defers) & jnp.logical_not(lends_relayed & late(i)))
        def _():
            y_copy(i).start()

        @pl.when(lends_own)
        def _():
            y_piece(i).start()

        return carry

    lax.fori_loop(0, CHUNKS, launch, 0)

    @pl.when(c == parity)
    def _():
        b_local.start()

    @pl.when(c != parity)
    def _():
        b_partner.start()

    @pl.when(lends_relayed)
    def _():
        e_own.start()

    @pl.when(lends_own)
    def _():
        for i in range(kept, CHUNKS):
            y_arrival(i).wait()
        e_relay.start()

        def lend(i, carry):
            x_own(i)
            return carry
        lax.fori_loop(0, CHUNKS, lend, 0)

    @pl.when(lends_own | helps)
    def _():
        y_sent(0).wait_send()
        pl.semaphore_signal(turn, inc=1, **other(**partner))

    def take_turn():
        pl.semaphore_wait(turn, 1)

        def cross(i, carry):
            y_copy(i).start()
            return carry
        lax.fori_loop(0, CHUNKS, cross, 0)

    @pl.when(yields)
    def _():
        take_turn()

    own_copy.wait()

    @pl.when(c == parity)
    def _():
        b_local.wait()
        b_sent(2).wait_recv()

    def b_arrival(s, u):
        ref = bbuf.at[s, :, :, fine_span(u), :]
        return pltpu.make_async_copy(ref, ref, brecv.at[s, u])

    def relay(s, u, part, row):
        ref = bbuf.at[s, :, :, fine_span(u), :]
        return pltpu.make_async_remote_copy(
            src_ref=ref, dst_ref=ref, send_sem=rsend.at[s, part], recv_sem=brecv.at[s, u],
            **other(row=row))

    def half_relay(s, n, row):
        ref = bbuf.at[s, (1 - c + n) % 2, :, late_span, :]
        return pltpu.make_async_remote_copy(
            src_ref=ref, dst_ref=ref, send_sem=rsend.at[s, 1],
            recv_sem=brecv.at[s, kept * FINE + n], **other(row=row))

    def relayed(s, part):
        start, size = ((0, kept) if part == 0 else (kept, EXTRA))
        ref = bbuf.at[s, :, :, pl.ds(start * step, size * step), :]
        return pltpu.make_async_remote_copy(
            src_ref=ref, dst_ref=ref, send_sem=rsend.at[s, part], recv_sem=brecv.at[s, 0],
            **other(row=inward))

    def present(s):
        quarter = 2 * s + c
        return jnp.logical_not((at_low & (quarter == 1)) | (at_high & (quarter == last - 1)))

    def is_own(s):
        return 2 * s + c == z

    def is_outer(s):
        outer = jnp.where(z < rows // 2, 0, last)
        return (2 * s + c == outer) & jnp.logical_not(at_end)

    def is_far(s):
        return 2 * s + c == far

    def goes_up(s):
        quarter = 2 * s + c
        return (quarter < z) & (z < last)

    def goes_down(s):
        quarter = 2 * s + c
        return (quarter > z) & (z > 0)

    def goes(s, i):
        cut = is_far(s) & ((z == 1) | (z == last - 1)) & late(i)
        return (goes_up(s) | goes_down(s)) & jnp.logical_not(cut)

    def split(value):
        high = value.astype(jnp.bfloat16)
        return high, (value - high.astype(jnp.float32)).astype(jnp.bfloat16)

    def dot(a, b):
        a_high, a_low = split(a)
        b_high, b_low = split(b)
        return jnp.dot(
            jnp.concatenate([a_high, a_high, a_low], axis=1),
            jnp.concatenate([b_high, b_low, b_high], axis=0),
            preferred_element_type=jnp.float32)

    def both(s, at):
        return (jnp.concatenate([bbuf[s, h, k, at, :] for h in range(2)], axis=1) for k in range(2))

    def accumulate(a_ref, s, at):
        a_re, a_im = a_ref[0, :, at], a_ref[1, :, at]
        b_re, b_im = both(s, at)
        acc[0] += dot(a_re, b_re)
        acc[1] += dot(a_im, b_im)
        acc[2] += dot(a_re + a_im, b_re + b_im)

    def multiply(a_ref, s, i):

        @pl.when((i % 2 == 1) & jnp.logical_not(at_end & is_far(s) & late(i)))
        def _():
            accumulate(a_ref, s, pl.ds(pl.multiple_of((i - 1) * step, 2 * step), 2 * step))

    def lent_step(i):
        def act(band, start, source, size):
            ref = xbuf.at[:, band, pl.ds(start, size)]
            pltpu.make_async_copy(ref, ref, xrecv.at[i]).wait()
            at = pl.ds(start, size)
            a_re, a_im = xbuf[0, band, at], xbuf[1, band, at]
            b_re, b_im = both(z // 2, at)
            xacc[0, band] += dot(a_re, b_re)
            xacc[1, band] += dot(a_im, b_im)
            xacc[2, band] += dot(a_re + a_im, b_re + b_im)
        by_piece(i, act)

    def combined(totals, h, g):
        first, second, third = (totals[k, group(g), half(h)] for k in range(3))
        return first - second, third - first - second

    def lend_back(h, b):
        return pltpu.make_async_remote_copy(
            src_ref=xout.at[h, :, band_of(b)], dst_ref=xin.at[:, band_of(b)],
            send_sem=csend.at[h], recv_sem=crecv.at[b], **other(row=outward, col=y * 2 + h))

    def lent_back(h):
        return pltpu.make_async_remote_copy(
            src_ref=xout.at[h], dst_ref=xin, send_sem=csend.at[h], recv_sem=crecv.at[0],
            **other(row=outward, col=y * 2 + h))

    def lent_arrival(b):
        ref = xin.at[:, band_of(b)]
        return pltpu.make_async_copy(ref, ref, crecv.at[b])

    def give(h, g):
        xout[h, 0, group(g)], xout[h, 1, group(g)] = combined(xacc, h, g)
        for k in range(per):
            lend_back(h, g * per + k).start()

    def extra_step(n):
        h = (1 - c + n) % 2
        b_re, b_im = (bbuf[1 - z // 2, h, k, late_span, :] for k in range(2))
        b_sum = b_re + b_im
        lanes = half(h)

        for g in range(GROUPS):
            band = group(g)
            a_re, a_im = ebuf[0, band, :], ebuf[1, band, :]
            xacc[0, band, lanes] += dot(a_re, b_re)
            xacc[1, band, lanes] += dot(a_im, b_im)
            xacc[2, band, lanes] += dot(a_re + a_im, b_sum)
            if g < GROUPS - 1:
                give(h, g)

    def banded(h, b):
        first, second, third = (acc[k, band_of(b), half(h)] for k in range(3))
        return first - second, third - first - second

    def to_partner(b):
        return pltpu.make_async_remote_copy(
            src_ref=pout.at[:, band_of(b)], dst_ref=pin.at[:, band_of(b)],
            send_sem=psend, recv_sem=precv.at[b], **other(**partner))

    def hand(b, carry):
        pout[0, band_of(b)], pout[1, band_of(b)] = banded(1 - c, b)
        to_partner(b).start()
        return carry

    def half_wait(n):
        s = 1 - z // 2
        ref = bbuf.at[s, (1 - c + n) % 2, :, late_span, :]
        pltpu.make_async_copy(ref, ref, brecv.at[s, kept * FINE + n]).wait()

    def half_product(n):
        s = 1 - z // 2
        h = (1 - c + n) % 2
        a_re, a_im = abuf[s, 0, :, late_span], abuf[s, 1, :, late_span]
        b_re, b_im = (bbuf[s, h, k, late_span, :] for k in range(2))
        lanes = half(h)
        acc[0, :, lanes] += dot(a_re, b_re)
        acc[1, :, lanes] += dot(a_im, b_im)
        acc[2, :, lanes] += dot(a_re + a_im, b_re + b_im)

    def half_step(i):
        @pl.when(i == kept)
        def _():
            for k in range(kept, CHUNKS):
                y_arrival(k).wait()
            e_own.wait_recv()
            half_wait(0)
            extra_step(0)
            half_product(0)
            accumulate(abuf.at[z // 2], z // 2, late_span)
            lax.fori_loop(0, BANDS, hand, 0)

        @pl.when(i == tail)
        def _():
            half_wait(1)
            extra_step(1)
            lent_step(i - LAG)
            lent_step(i)
            for h in range(2):
                give(h, GROUPS - 1)
            half_product(1)

    def right_step(i):
        @pl.when(defers & (i == kept))
        def _():
            take_turn()

        for order in range(2):
            s = jnp.where(z < rows // 2, 1 - order, order)

            @pl.when(present(s) & jnp.logical_not(is_own(s)) & jnp.logical_not(at_end & is_far(s) & late(i)))
            def _():
                onward = jnp.where(goes_up(s), z + 1, z - 1)
                in_halves = late(i) & helps & is_far(s)
                by_halves = late(i) & is_outer(s)

                @pl.when(jnp.logical_not(in_halves))
                def _():
                    for k in range(FINE):
                        b_arrival(s, i * FINE + k).wait()

                        @pl.when(goes(s, i) & jnp.logical_not(by_halves))
                        def _():
                            relay(s, i * FINE + k, late(i).astype(jnp.int32), onward).start()

                @pl.when(by_halves & (i == tail))
                def _():
                    for n in range(2):
                        half_relay(s, n, onward).start()

        @pl.when(helps & late(i))
        def _():
            half_step(i)

        @pl.when(lends & (i == 0))
        def _():
            for u in range(FILL * FINE):
                b_arrival(lent_slot, u).wait()
            accumulate(abuf.at[lent_slot], lent_slot, pl.ds(0, fill))

        @pl.when(present(y) & jnp.logical_not(helps & late(i)))
        def _():
            multiply(abuf.at[y], y, i)

    def left_step(i):
        @pl.when(jnp.logical_not(lends_relayed | ((lends_own | helps) & late(i))))
        def _():
            y_arrival(i).wait()

        @pl.when(lends_relayed)
        def _():
            y_piece_arrival(i).wait()
            x_relay(i)

        @pl.when(present(1 - y) & jnp.logical_not(helps & late(i)))
        def _():
            multiply(abuf.at[1 - y], 1 - y, i)

        @pl.when(helps & (i >= LAG) & (i < tail))
        def _():
            lent_step(i - LAG)

    early = jnp.logical_not(at_end) & (c != parity)

    def work(t, carry):
        first = t < CHUNKS
        apart = jnp.where(first, t, t - CHUNKS)
        i = jnp.where(early | lends_relayed, apart, t // 2)
        is_left = ((early & jnp.logical_not(first)) | (lends_relayed & first)
                   | (jnp.logical_not(early | lends_relayed) & (t % 2 == 1)))

        @pl.when(is_left)
        def _():
            left_step(i)

        @pl.when(jnp.logical_not(is_left))
        def _():
            right_step(i)

        return carry

    lax.fori_loop(0, 2 * CHUNKS, work, 0)

    def to_copy(b):
        return pltpu.make_async_remote_copy(
            src_ref=qout.at[:, band_of(b)], dst_ref=qin.at[:, band_of(b)],
            send_sem=qsend, recv_sem=qrecv, **other(**copy_x))

    @pl.when(jnp.logical_not(helps))
    def _():
        lax.fori_loop(0, BANDS, hand, 0)

    def gather(b, carry):
        band = band_of(b)
        mine_re, mine_im = banded(c, b)
        to_partner(b).wait_recv()
        qout[0, band] = mine_re + pin[0, band]
        qout[1, band] = mine_im + pin[1, band]

        @pl.when(at_end)
        def _():
            lent_arrival(b).wait()
            qout[:, band] += xin[:, band]

        to_copy(b).start()
        return carry

    lax.fori_loop(0, BANDS, gather, 0)

    @pl.when(sends_up)
    def _():
        b_sent(0).wait_send()

    @pl.when(sends_down)
    def _():
        b_sent(1).wait_send()

    @pl.when(c != parity)
    def _():
        b_partner.wait_send()

    @pl.when(fills_down | fills_up)
    def _():
        ref = bbuf.at[z // 2, c, :, pl.ds(0, fill), :]
        pltpu.make_async_remote_copy(
            src_ref=ref, dst_ref=ref, send_sem=bsend.at[3], recv_sem=bown.at[1],
            **other(**partner)).wait_send()

    @pl.when(jnp.logical_not(lends_own | helps))
    def _():
        y_sent(0).wait_send()

    y_sent(1).wait_send()

    @pl.when(lends)
    def _():
        x_sent.wait_send()
        e_own.wait_send()

    for s in range(2):
        for part in range(2):
            @pl.when(present(s) & goes(s, tail * part))
            def _():
                relayed(s, part).wait_send()

    @pl.when(helps)
    def _():
        for h in range(2):
            lent_back(h).wait_send()

    whole_part = pltpu.make_async_remote_copy(
        src_ref=pout, dst_ref=pin, send_sem=psend, recv_sem=precv.at[0], **other(**partner))
    whole_part.wait_send()

    whole_copy = pltpu.make_async_remote_copy(
        src_ref=qout, dst_ref=qin, send_sem=qsend, recv_sem=qrecv, **other(**copy_x))
    whole_copy.wait()


def lent_product(left_matrix, right_matrix, layers, rows):
    height = left_matrix.shape[1]
    width = right_matrix.shape[2]
    share = left_matrix.shape[2] // layers
    f32 = jnp.float32
    dma = pltpu.SemaphoreType.DMA
    block = (2, height, width)
    own, copied = pl.pallas_call(
        functools.partial(kernel, rows),
        out_shape=[pltpu.VMEM(block, f32)] * 2,
        in_specs=[pl.BlockSpec(memory_space=pl.ANY)] * 2,
        out_specs=[pl.BlockSpec(memory_space=pltpu.VMEM)] * 2,
        scratch_shapes=[
            pltpu.VMEM((2, 2, height, share), f32),
            pltpu.VMEM((2, 2, 2, share, width), f32),
            pltpu.VMEM((2, height, share), f32),
            pltpu.VMEM((2, height, EXTRA * share // CHUNKS), f32),
            pltpu.VMEM((3, height, 2 * width), f32),
            pltpu.VMEM((3, height, 2 * width), f32),
            pltpu.VMEM((2,) + block, f32),
            pltpu.VMEM(block, f32),
            pltpu.VMEM(block, f32),
            pltpu.VMEM(block, f32),
            dma,
            dma((4,)),
            dma((2, 2)),
            dma((2, CHUNKS * FINE)),
            dma((2,)),
            dma((2,)),
            dma((CHUNKS,)),
            dma,
            dma((CHUNKS,)),
            dma((2,)),
            dma((2,)),
            dma((BANDS,)),
            dma,
            dma((BANDS,)),
            dma,
            dma,
            pltpu.SemaphoreType.REGULAR,
        ],
        compiler_params=pltpu.CompilerParams(
            collective_id=0, has_side_effects=True, vmem_limit_bytes=60 * 2**20),
    )(left_matrix, right_matrix)
    return own + copied


def gathered_product(left_matrix, right_matrix, layers):
    layer_index = lax.axis_index("layer")
    local_cols = right_matrix.shape[2]
    left_width = left_matrix.shape[2]
    right_height = right_matrix.shape[1]
    share_width = left_width // layers
    group_count = right_height // left_width
    left_own = lax.dynamic_slice_in_dim(left_matrix, layer_index * share_width, share_width, 2)
    right_view = right_matrix.reshape(2, group_count, layers, share_width, local_cols)
    right_own = lax.dynamic_slice_in_dim(right_view, layer_index, 1, 2)
    right_own = right_own.reshape(2, group_count * share_width, local_cols)
    right_whole = lax.all_gather(right_own, "row", axis=1, tiled=True)
    left_whole = lax.all_gather(left_own, "col", axis=2, tiled=True)
    dot = functools.partial(
        jnp.dot, precision=lax.Precision.HIGHEST, preferred_element_type=jnp.float32)
    first_term = dot(left_whole[0], right_whole[0])
    second_term = dot(left_whole[1], right_whole[1])
    third_term = dot(left_whole[0] + left_whole[1], right_whole[0] + right_whole[1])
    partial_product = jnp.stack([first_term - second_term, third_term - first_term - second_term])
    return lax.psum(partial_product, "layer")


def local(left_matrix, right_matrix):
    layers = lax.axis_size("layer")
    rows = lax.axis_size("row")
    cols = lax.axis_size("col")
    if layers == 2 and rows == cols == 4:
        return lent_product(left_matrix, right_matrix, layers, rows)
    return gathered_product(left_matrix, right_matrix, layers)


def solution(mesh):
    in_specs = (P(None, "row", "col"), P(None, "row", "col"))
    out_specs = P(None, "row", "col")
    return jax.shard_map(local, mesh=mesh, in_specs=in_specs, out_specs=out_specs, check_vma=False)
```

```python
import functools

import jax
import jax.numpy as jnp
from jax import lax
from jax.experimental import pallas as pl
from jax.experimental.pallas import tpu as pltpu
from jax.sharding import PartitionSpec as P

CHUNKS = 16
FINE = 2
GROUPS = 4
EXTRA = 2
FILL = 2
LAG = 1
BANDS = 8
MESH = pl.DeviceIdType.MESH


def kernel(rows, left, right, qout, qin, abuf, bbuf, xbuf, ebuf, acc, xacc, xout, xin, pout, pin,
           own_sem, bsend, rsend, brecv, bown, ysend, yrecv, xsend, xrecv, esem, csend, crecv,
           psend, precv, qsend, qrecv, turn):
    x = lax.axis_index("layer")
    z = lax.axis_index("row")
    col = lax.axis_index("col")
    y = col // 2
    c = col % 2
    height = left.shape[1]
    width = right.shape[2]
    share = abuf.shape[3]
    step = share // CHUNKS
    fine = step // FINE
    tall = height // GROUPS
    parts = CHUNKS // GROUPS
    wide = share // parts
    fill = FILL * step
    last = rows - 1
    tail = CHUNKS - 1
    kept = CHUNKS - EXTRA
    base = x * share
    parity = z % 2
    at_low, at_high = z == 0, z == last
    at_end = at_low | at_high
    lends = (at_low & (c == 1)) | (at_high & (c == 0))
    helps = ((z == 1) & (c == 1)) | ((z == last - 1) & (c == 0))
    inward = jnp.where(at_low, 1, last - 1)
    outward = jnp.where(z == 1, 0, last)
    far = jnp.where(z < rows // 2, last, 0)
    lent_slot = jnp.where(at_low, 0, (last - 1) // 2)
    lends_own = lends & (y == lent_slot)
    lends_relayed = lends & (y != lent_slot)

    def other(**where):
        return dict(device_id=where, device_id_type=MESH)

    partner = dict(col=y * 2 + 1 - c)
    across = dict(col=(1 - y) * 2 + c)
    copy_x = dict(layer=1 - x)

    barrier = pltpu.get_barrier_semaphore()
    for where in (partner, across, copy_x):
        pl.semaphore_signal(barrier, inc=1, **other(**where))

    @pl.when(z > 0)
    def _():
        for core in range(2):
            pl.semaphore_signal(barrier, inc=1, **other(row=z - 1, col=y * 2 + core))

    @pl.when(z < last)
    def _():
        for core in range(2):
            pl.semaphore_signal(barrier, inc=1, **other(row=z + 1, col=y * 2 + core))

    own_copy = pltpu.make_async_copy(left.at[:, :, pl.ds(base, share)], abuf.at[y], own_sem)
    own_copy.start()
    acc[...] = jnp.zeros_like(acc)
    xacc[...] = jnp.zeros_like(xacc)
    pl.semaphore_wait(barrier, 3 + 2 * ((z > 0).astype(jnp.int32) + (z < last).astype(jnp.int32)))

    def span(i):
        return pl.ds(pl.multiple_of(i * step, step), step)

    def source_span(i):
        return pl.ds(pl.multiple_of(base + i * step, step), step)

    def fine_span(u):
        return pl.ds(pl.multiple_of(u * fine, fine), fine)

    def fine_source(u):
        return pl.ds(pl.multiple_of(base + u * fine, fine), fine)

    def half(h):
        return pl.ds(pl.multiple_of(h * width, width), width)

    thin = height // BANDS
    per = BANDS // GROUPS

    def band_of(b):
        return pl.ds(pl.multiple_of(b * thin, thin), thin)

    def group(g):
        return pl.ds(pl.multiple_of(g * tall, tall), tall)

    def piece_rows(i):
        return group(i // parts)

    def piece_cols(i):
        return pl.ds(pl.multiple_of((i % parts) * wide, wide), wide)

    def piece_source(i):
        return pl.ds(pl.multiple_of(base + (i % parts) * wide, step), wide)

    whole_source = pl.ds(pl.multiple_of(base, step), share)

    def b_copy(u, way, row):
        return pltpu.make_async_remote_copy(
            src_ref=right.at[:, fine_source(u), :],
            dst_ref=bbuf.at[z // 2, c, :, fine_span(u), :],
            send_sem=bsend.at[way], recv_sem=brecv.at[z // 2, u],
            **other(row=row, col=y * 2 + parity))

    def b_sent(way):
        return pltpu.make_async_remote_copy(
            src_ref=right.at[:, whole_source, :], dst_ref=bbuf.at[z // 2, c],
            send_sem=bsend.at[way], recv_sem=bown.at[1], **other(**partner))

    b_local = pltpu.make_async_copy(right.at[:, whole_source, :], bbuf.at[z // 2, c], bown.at[0])
    b_partner = b_sent(2)

    def y_part(i):
        return (i == tail).astype(jnp.int32) if not isinstance(i, int) else int(i == tail)

    def y_copy(i):
        return pltpu.make_async_remote_copy(
            src_ref=left.at[:, :, source_span(i)], dst_ref=abuf.at[y, :, :, span(i)],
            send_sem=ysend.at[y_part(i)], recv_sem=yrecv.at[i], **other(**across))

    def y_piece(i):
        return pltpu.make_async_remote_copy(
            src_ref=left.at[:, piece_rows(i), piece_source(i)],
            dst_ref=abuf.at[y, :, piece_rows(i), piece_cols(i)],
            send_sem=ysend.at[y_part(i)], recv_sem=yrecv.at[i], **other(**across))

    def late(i):
        return i >= kept

    late_span = pl.ds(kept * step, EXTRA * step)
    late_source = pl.ds(pl.multiple_of(base + kept * step, step), EXTRA * step)

    def y_sent(part):
        size = (tail if part == 0 else 1) * step
        ref = abuf.at[y, :, :, pl.ds(0, size)]
        return pltpu.make_async_remote_copy(
            src_ref=ref, dst_ref=ref, send_sem=ysend.at[part], recv_sem=yrecv.at[0], **other(**across))

    def y_arrival(i):
        ref = abuf.at[1 - y, :, :, span(i)]
        return pltpu.make_async_copy(ref, ref, yrecv.at[i])

    def y_piece_arrival(i):
        ref = abuf.at[1 - y, :, piece_rows(i), piece_cols(i)]
        return pltpu.make_async_copy(ref, ref, yrecv.at[i])

    def by_piece(i, act):
        @pl.when(i % parts == 0)
        def _():
            act(piece_rows(i), fill, pl.multiple_of(base + fill, step), wide - fill)

        @pl.when(i % parts != 0)
        def _():
            start = pl.multiple_of((i % parts) * wide, wide)
            act(piece_rows(i), start, pl.multiple_of(base + start, step), wide)

    def x_own(i):
        def act(band, start, source, size):
            pltpu.make_async_remote_copy(
                src_ref=left.at[:, band, pl.ds(source, size)],
                dst_ref=xbuf.at[:, band, pl.ds(start, size)],
                send_sem=xsend, recv_sem=xrecv.at[i], **other(row=inward)).start()
        by_piece(i, act)

    def x_relay(i):
        def act(band, start, source, size):
            pltpu.make_async_remote_copy(
                src_ref=abuf.at[1 - y, :, band, pl.ds(start, size)],
                dst_ref=xbuf.at[:, band, pl.ds(start, size)],
                send_sem=xsend, recv_sem=xrecv.at[i], **other(row=inward)).start()
        by_piece(i, act)

    lent_ref = xbuf.at[:, :, pl.ds(fill, share - fill)]
    x_sent = pltpu.make_async_remote_copy(
        src_ref=lent_ref, dst_ref=lent_ref, send_sem=xsend, recv_sem=xrecv.at[0], **other(row=inward))
    e_own = pltpu.make_async_remote_copy(
        src_ref=left.at[:, :, late_source], dst_ref=ebuf,
        send_sem=esem.at[0], recv_sem=esem.at[1], **other(row=inward))
    e_relay = pltpu.make_async_remote_copy(
        src_ref=abuf.at[1 - y, :, :, late_span], dst_ref=ebuf,
        send_sem=esem.at[0], recv_sem=esem.at[1], **other(row=inward))

    defers = jnp.logical_not(at_end | helps)
    yields = at_end & jnp.logical_not(lends) & (y == lent_slot)
    sends_up = (z < last) & (z != last - 1)
    sends_down = (z > 0) & (z != 1)

    fills_down = z == 1
    fills_up = z == last - 1
    fill_row = jnp.where(fills_down, 0, last)

    @pl.when(fills_down | fills_up)
    def _():
        for u in range(FILL * FINE):
            b_copy(u, 3, fill_row).start()

    @pl.when(lends_relayed)
    def _():
        for i in range(kept, CHUNKS):
            y_copy(i).start()

    def launch(i, carry):
        for k in range(FINE):
            @pl.when(sends_up)
            def _():
                b_copy(i * FINE + k, 0, z + 1).start()

            @pl.when(sends_down)
            def _():
                b_copy(i * FINE + k, 1, z - 1).start()

        @pl.when(jnp.logical_not(yields | lends_own | defers) & jnp.logical_not(lends_relayed & late(i)))
        def _():
            y_copy(i).start()

        @pl.when(lends_own)
        def _():
            y_piece(i).start()

        return carry

    lax.fori_loop(0, CHUNKS, launch, 0)

    @pl.when(c == parity)
    def _():
        b_local.start()

    @pl.when(c != parity)
    def _():
        b_partner.start()

    @pl.when(lends_relayed)
    def _():
        e_own.start()

    @pl.when(lends_own)
    def _():
        for i in range(kept, CHUNKS):
            y_arrival(i).wait()
        e_relay.start()

        def lend(i, carry):
            x_own(i)
            return carry
        lax.fori_loop(0, CHUNKS, lend, 0)

    @pl.when(lends_own | helps)
    def _():
        y_sent(0).wait_send()
        pl.semaphore_signal(turn, inc=1, **other(**partner))

    def take_turn():
        pl.semaphore_wait(turn, 1)

        def cross(i, carry):
            y_copy(i).start()
            return carry
        lax.fori_loop(0, CHUNKS, cross, 0)

    @pl.when(yields)
    def _():
        take_turn()

    own_copy.wait()

    @pl.when(c == parity)
    def _():
        b_local.wait()
        b_sent(2).wait_recv()

    def b_arrival(s, u):
        ref = bbuf.at[s, :, :, fine_span(u), :]
        return pltpu.make_async_copy(ref, ref, brecv.at[s, u])

    def relay(s, u, part, row):
        ref = bbuf.at[s, :, :, fine_span(u), :]
        return pltpu.make_async_remote_copy(
            src_ref=ref, dst_ref=ref, send_sem=rsend.at[s, part], recv_sem=brecv.at[s, u],
            **other(row=row))

    def half_relay(s, n, row):
        ref = bbuf.at[s, (1 - c + n) % 2, :, late_span, :]
        return pltpu.make_async_remote_copy(
            src_ref=ref, dst_ref=ref, send_sem=rsend.at[s, 1],
            recv_sem=brecv.at[s, kept * FINE + n], **other(row=row))

    def relayed(s, part):
        start, size = ((0, kept) if part == 0 else (kept, EXTRA))
        ref = bbuf.at[s, :, :, pl.ds(start * step, size * step), :]
        return pltpu.make_async_remote_copy(
            src_ref=ref, dst_ref=ref, send_sem=rsend.at[s, part], recv_sem=brecv.at[s, 0],
            **other(row=inward))

    def present(s):
        quarter = 2 * s + c
        return jnp.logical_not((at_low & (quarter == 1)) | (at_high & (quarter == last - 1)))

    def is_own(s):
        return 2 * s + c == z

    def is_outer(s):
        outer = jnp.where(z < rows // 2, 0, last)
        return (2 * s + c == outer) & jnp.logical_not(at_end)

    def is_far(s):
        return 2 * s + c == far

    def goes_up(s):
        quarter = 2 * s + c
        return (quarter < z) & (z < last)

    def goes_down(s):
        quarter = 2 * s + c
        return (quarter > z) & (z > 0)

    def goes(s, i):
        cut = is_far(s) & ((z == 1) | (z == last - 1)) & late(i)
        return (goes_up(s) | goes_down(s)) & jnp.logical_not(cut)

    def split(value):
        high = value.astype(jnp.bfloat16)
        return high, (value - high.astype(jnp.float32)).astype(jnp.bfloat16)

    def dot(a, b):
        a_high, a_low = split(a)
        b_high, b_low = split(b)
        return jnp.dot(
            jnp.concatenate([a_high, a_high, a_low], axis=1),
            jnp.concatenate([b_high, b_low, b_high], axis=0),
            preferred_element_type=jnp.float32)

    def both(s, at):
        return (jnp.concatenate([bbuf[s, h, k, at, :] for h in range(2)], axis=1) for k in range(2))

    def accumulate(a_ref, s, at):
        a_re, a_im = a_ref[0, :, at], a_ref[1, :, at]
        b_re, b_im = both(s, at)
        acc[0] += dot(a_re, b_re)
        acc[1] += dot(a_im, b_im)
        acc[2] += dot(a_re + a_im, b_re + b_im)

    def multiply(a_ref, s, i):

        @pl.when((i % 2 == 1) & jnp.logical_not(at_end & is_far(s) & late(i)))
        def _():
            accumulate(a_ref, s, pl.ds(pl.multiple_of((i - 1) * step, 2 * step), 2 * step))

    def lent_step(i):
        def act(band, start, source, size):
            ref = xbuf.at[:, band, pl.ds(start, size)]
            pltpu.make_async_copy(ref, ref, xrecv.at[i]).wait()
            at = pl.ds(start, size)
            a_re, a_im = xbuf[0, band, at], xbuf[1, band, at]
            b_re, b_im = both(z // 2, at)
            xacc[0, band] += dot(a_re, b_re)
            xacc[1, band] += dot(a_im, b_im)
            xacc[2, band] += dot(a_re + a_im, b_re + b_im)
        by_piece(i, act)

    def combined(totals, h, g):
        first, second, third = (totals[k, group(g), half(h)] for k in range(3))
        return first - second, third - first - second

    def lend_back(h, b):
        return pltpu.make_async_remote_copy(
            src_ref=xout.at[h, :, band_of(b)], dst_ref=xin.at[:, band_of(b)],
            send_sem=csend.at[h], recv_sem=crecv.at[b], **other(row=outward, col=y * 2 + h))

    def lent_back(h):
        return pltpu.make_async_remote_copy(
            src_ref=xout.at[h], dst_ref=xin, send_sem=csend.at[h], recv_sem=crecv.at[0],
            **other(row=outward, col=y * 2 + h))

    def lent_arrival(b):
        ref = xin.at[:, band_of(b)]
        return pltpu.make_async_copy(ref, ref, crecv.at[b])

    def give(h, g):
        xout[h, 0, group(g)], xout[h, 1, group(g)] = combined(xacc, h, g)
        for k in range(per):
            lend_back(h, g * per + k).start()

    def extra_step(n):
        h = (1 - c + n) % 2
        b_re, b_im = (bbuf[1 - z // 2, h, k, late_span, :] for k in range(2))
        b_sum = b_re + b_im
        lanes = half(h)

        for g in range(GROUPS):
            band = group(g)
            a_re, a_im = ebuf[0, band, :], ebuf[1, band, :]
            xacc[0, band, lanes] += dot(a_re, b_re)
            xacc[1, band, lanes] += dot(a_im, b_im)
            xacc[2, band, lanes] += dot(a_re + a_im, b_sum)
            if g < GROUPS - 1:
                give(h, g)

    def banded(h, b):
        first, second, third = (acc[k, band_of(b), half(h)] for k in range(3))
        return first - second, third - first - second

    def to_partner(b):
        return pltpu.make_async_remote_copy(
            src_ref=pout.at[:, band_of(b)], dst_ref=pin.at[:, band_of(b)],
            send_sem=psend, recv_sem=precv.at[b], **other(**partner))

    def hand(b, carry):
        pout[0, band_of(b)], pout[1, band_of(b)] = banded(1 - c, b)
        to_partner(b).start()
        return carry

    def half_wait(n):
        s = 1 - z // 2
        ref = bbuf.at[s, (1 - c + n) % 2, :, late_span, :]
        pltpu.make_async_copy(ref, ref, brecv.at[s, kept * FINE + n]).wait()

    def half_product(n):
        s = 1 - z // 2
        h = (1 - c + n) % 2
        a_re, a_im = abuf[s, 0, :, late_span], abuf[s, 1, :, late_span]
        b_re, b_im = (bbuf[s, h, k, late_span, :] for k in range(2))
        lanes = half(h)
        acc[0, :, lanes] += dot(a_re, b_re)
        acc[1, :, lanes] += dot(a_im, b_im)
        acc[2, :, lanes] += dot(a_re + a_im, b_re + b_im)

    def half_step(i):
        @pl.when(i == kept)
        def _():
            for k in range(kept, CHUNKS):
                y_arrival(k).wait()
            e_own.wait_recv()
            half_wait(0)
            extra_step(0)
            half_product(0)
            accumulate(abuf.at[z // 2], z // 2, late_span)
            lax.fori_loop(0, BANDS, hand, 0)

        @pl.when(i == tail)
        def _():
            half_wait(1)
            extra_step(1)
            lent_step(i - LAG)
            lent_step(i)
            for h in range(2):
                give(h, GROUPS - 1)
            half_product(1)

    def right_step(i):
        @pl.when(defers & (i == kept))
        def _():
            take_turn()

        for order in range(2):
            s = jnp.where(z < rows // 2, 1 - order, order)

            @pl.when(present(s) & jnp.logical_not(is_own(s)) & jnp.logical_not(at_end & is_far(s) & late(i)))
            def _():
                onward = jnp.where(goes_up(s), z + 1, z - 1)
                in_halves = late(i) & helps & is_far(s)
                by_halves = late(i) & is_outer(s)

                @pl.when(jnp.logical_not(in_halves))
                def _():
                    for k in range(FINE):
                        b_arrival(s, i * FINE + k).wait()

                        @pl.when(goes(s, i) & jnp.logical_not(by_halves))
                        def _():
                            relay(s, i * FINE + k, late(i).astype(jnp.int32), onward).start()

                @pl.when(by_halves & (i == tail))
                def _():
                    for n in range(2):
                        half_relay(s, n, onward).start()

        @pl.when(helps & late(i))
        def _():
            half_step(i)

        @pl.when(lends & (i == 0))
        def _():
            for u in range(FILL * FINE):
                b_arrival(lent_slot, u).wait()
            accumulate(abuf.at[lent_slot], lent_slot, pl.ds(0, fill))

        @pl.when(present(y) & jnp.logical_not(helps & late(i)))
        def _():
            multiply(abuf.at[y], y, i)

        @pl.when(lends_relayed & (i == kept - 1))
        def _():
            lax.fori_loop(0, BANDS, hand, 0)

    def left_step(i):
        @pl.when(jnp.logical_not(lends_relayed | ((lends_own | helps) & late(i))))
        def _():
            y_arrival(i).wait()

        @pl.when(lends_relayed)
        def _():
            y_piece_arrival(i).wait()
            x_relay(i)

        @pl.when(present(1 - y) & jnp.logical_not(helps & late(i)))
        def _():
            multiply(abuf.at[1 - y], 1 - y, i)

        @pl.when(lends_own & (i == kept - 1))
        def _():
            lax.fori_loop(0, BANDS, hand, 0)

        @pl.when(helps & (i >= LAG) & (i < tail))
        def _():
            lent_step(i - LAG)

    early = jnp.logical_not(at_end) & (c != parity)

    def work(t, carry):
        first = t < CHUNKS
        apart = jnp.where(first, t, t - CHUNKS)
        i = jnp.where(early | lends_relayed, apart, t // 2)
        is_left = ((early & jnp.logical_not(first)) | (lends_relayed & first)
                   | (jnp.logical_not(early | lends_relayed) & (t % 2 == 1)))

        @pl.when(is_left)
        def _():
            left_step(i)

        @pl.when(jnp.logical_not(is_left))
        def _():
            right_step(i)

        return carry

    lax.fori_loop(0, 2 * CHUNKS, work, 0)

    def to_copy(b):
        return pltpu.make_async_remote_copy(
            src_ref=qout.at[:, band_of(b)], dst_ref=qin.at[:, band_of(b)],
            send_sem=qsend, recv_sem=qrecv, **other(**copy_x))

    @pl.when(jnp.logical_not(helps | lends))
    def _():
        lax.fori_loop(0, BANDS, hand, 0)

    def gather(b, carry):
        band = band_of(b)
        mine_re, mine_im = banded(c, b)
        to_partner(b).wait_recv()
        qout[0, band] = mine_re + pin[0, band]
        qout[1, band] = mine_im + pin[1, band]

        @pl.when(at_end)
        def _():
            lent_arrival(b).wait()
            qout[:, band] += xin[:, band]

        to_copy(b).start()
        return carry

    lax.fori_loop(0, BANDS, gather, 0)

    @pl.when(sends_up)
    def _():
        b_sent(0).wait_send()

    @pl.when(sends_down)
    def _():
        b_sent(1).wait_send()

    @pl.when(c != parity)
    def _():
        b_partner.wait_send()

    @pl.when(fills_down | fills_up)
    def _():
        ref = bbuf.at[z // 2, c, :, pl.ds(0, fill), :]
        pltpu.make_async_remote_copy(
            src_ref=ref, dst_ref=ref, send_sem=bsend.at[3], recv_sem=bown.at[1],
            **other(**partner)).wait_send()

    @pl.when(jnp.logical_not(lends_own | helps))
    def _():
        y_sent(0).wait_send()

    y_sent(1).wait_send()

    @pl.when(lends)
    def _():
        x_sent.wait_send()
        e_own.wait_send()

    for s in range(2):
        for part in range(2):
            @pl.when(present(s) & goes(s, tail * part))
            def _():
                relayed(s, part).wait_send()

    @pl.when(helps)
    def _():
        for h in range(2):
            lent_back(h).wait_send()

    whole_part = pltpu.make_async_remote_copy(
        src_ref=pout, dst_ref=pin, send_sem=psend, recv_sem=precv.at[0], **other(**partner))
    whole_part.wait_send()

    whole_copy = pltpu.make_async_remote_copy(
        src_ref=qout, dst_ref=qin, send_sem=qsend, recv_sem=qrecv, **other(**copy_x))
    whole_copy.wait()


def lent_product(left_matrix, right_matrix, layers, rows):
    height = left_matrix.shape[1]
    width = right_matrix.shape[2]
    share = left_matrix.shape[2] // layers
    f32 = jnp.float32
    dma = pltpu.SemaphoreType.DMA
    block = (2, height, width)
    own, copied = pl.pallas_call(
        functools.partial(kernel, rows),
        out_shape=[pltpu.VMEM(block, f32)] * 2,
        in_specs=[pl.BlockSpec(memory_space=pl.ANY)] * 2,
        out_specs=[pl.BlockSpec(memory_space=pltpu.VMEM)] * 2,
        scratch_shapes=[
            pltpu.VMEM((2, 2, height, share), f32),
            pltpu.VMEM((2, 2, 2, share, width), f32),
            pltpu.VMEM((2, height, share), f32),
            pltpu.VMEM((2, height, EXTRA * share // CHUNKS), f32),
            pltpu.VMEM((3, height, 2 * width), f32),
            pltpu.VMEM((3, height, 2 * width), f32),
            pltpu.VMEM((2,) + block, f32),
            pltpu.VMEM(block, f32),
            pltpu.VMEM(block, f32),
            pltpu.VMEM(block, f32),
            dma,
            dma((4,)),
            dma((2, 2)),
            dma((2, CHUNKS * FINE)),
            dma((2,)),
            dma((2,)),
            dma((CHUNKS,)),
            dma,
            dma((CHUNKS,)),
            dma((2,)),
            dma((2,)),
            dma((BANDS,)),
            dma,
            dma((BANDS,)),
            dma,
            dma,
            pltpu.SemaphoreType.REGULAR,
        ],
        compiler_params=pltpu.CompilerParams(
            collective_id=0, has_side_effects=True, vmem_limit_bytes=60 * 2**20),
    )(left_matrix, right_matrix)
    return own + copied


def gathered_product(left_matrix, right_matrix, layers):
    layer_index = lax.axis_index("layer")
    local_cols = right_matrix.shape[2]
    left_width = left_matrix.shape[2]
    right_height = right_matrix.shape[1]
    share_width = left_width // layers
    group_count = right_height // left_width
    left_own = lax.dynamic_slice_in_dim(left_matrix, layer_index * share_width, share_width, 2)
    right_view = right_matrix.reshape(2, group_count, layers, share_width, local_cols)
    right_own = lax.dynamic_slice_in_dim(right_view, layer_index, 1, 2)
    right_own = right_own.reshape(2, group_count * share_width, local_cols)
    right_whole = lax.all_gather(right_own, "row", axis=1, tiled=True)
    left_whole = lax.all_gather(left_own, "col", axis=2, tiled=True)
    dot = functools.partial(
        jnp.dot, precision=lax.Precision.HIGHEST, preferred_element_type=jnp.float32)
    first_term = dot(left_whole[0], right_whole[0])
    second_term = dot(left_whole[1], right_whole[1])
    third_term = dot(left_whole[0] + left_whole[1], right_whole[0] + right_whole[1])
    partial_product = jnp.stack([first_term - second_term, third_term - first_term - second_term])
    return lax.psum(partial_product, "layer")


def local(left_matrix, right_matrix):
    layers = lax.axis_size("layer")
    rows = lax.axis_size("row")
    cols = lax.axis_size("col")
    if layers == 2 and rows == cols == 4:
        return lent_product(left_matrix, right_matrix, layers, rows)
    return gathered_product(left_matrix, right_matrix, layers)


def solution(mesh):
    in_specs = (P(None, "row", "col"), P(None, "row", "col"))
    out_specs = P(None, "row", "col")
    return jax.shard_map(local, mesh=mesh, in_specs=in_specs, out_specs=out_specs, check_vma=False)
```

```python
import functools

import jax
import jax.numpy as jnp
from jax import lax
from jax.experimental import pallas as pl
from jax.experimental.pallas import tpu as pltpu
from jax.sharding import PartitionSpec as P

CHUNKS = 16
FINE = 2
GROUPS = 4
EXTRA = 2
FILL = 2
LAG = 1
BANDS = 8
MESH = pl.DeviceIdType.MESH


def kernel(rows, left, right, qout, qin, abuf, bbuf, xbuf, ebuf, acc, xacc, xout, xin, pout, pin,
           own_sem, bsend, rsend, brecv, bown, ysend, yrecv, xsend, xrecv, esem, csend, crecv,
           psend, precv, qsend, qrecv, turn):
    x = lax.axis_index("layer")
    z = lax.axis_index("row")
    col = lax.axis_index("col")
    y = col // 2
    c = col % 2
    height = left.shape[1]
    width = right.shape[2]
    share = abuf.shape[3]
    step = share // CHUNKS
    fine = step // FINE
    tall = height // GROUPS
    parts = CHUNKS // GROUPS
    wide = share // parts
    fill = FILL * step
    last = rows - 1
    tail = CHUNKS - 1
    kept = CHUNKS - EXTRA
    base = x * share
    parity = z % 2
    at_low, at_high = z == 0, z == last
    at_end = at_low | at_high
    lends = (at_low & (c == 1)) | (at_high & (c == 0))
    helps = ((z == 1) & (c == 1)) | ((z == last - 1) & (c == 0))
    inward = jnp.where(at_low, 1, last - 1)
    outward = jnp.where(z == 1, 0, last)
    far = jnp.where(z < rows // 2, last, 0)
    lent_slot = jnp.where(at_low, 0, (last - 1) // 2)
    lends_own = lends & (y == lent_slot)
    lends_relayed = lends & (y != lent_slot)

    def other(**where):
        return dict(device_id=where, device_id_type=MESH)

    partner = dict(col=y * 2 + 1 - c)
    across = dict(col=(1 - y) * 2 + c)
    copy_x = dict(layer=1 - x)

    barrier = pltpu.get_barrier_semaphore()
    for where in (partner, across, copy_x):
        pl.semaphore_signal(barrier, inc=1, **other(**where))

    @pl.when(z > 0)
    def _():
        for core in range(2):
            pl.semaphore_signal(barrier, inc=1, **other(row=z - 1, col=y * 2 + core))

    @pl.when(z < last)
    def _():
        for core in range(2):
            pl.semaphore_signal(barrier, inc=1, **other(row=z + 1, col=y * 2 + core))

    own_copy = pltpu.make_async_copy(left.at[:, :, pl.ds(base, share)], abuf.at[y], own_sem)
    own_copy.start()
    acc[...] = jnp.zeros_like(acc)
    xacc[...] = jnp.zeros_like(xacc)
    pl.semaphore_wait(barrier, 3 + 2 * ((z > 0).astype(jnp.int32) + (z < last).astype(jnp.int32)))

    def span(i):
        return pl.ds(pl.multiple_of(i * step, step), step)

    def source_span(i):
        return pl.ds(pl.multiple_of(base + i * step, step), step)

    def fine_span(u):
        return pl.ds(pl.multiple_of(u * fine, fine), fine)

    def fine_source(u):
        return pl.ds(pl.multiple_of(base + u * fine, fine), fine)

    def half(h):
        return pl.ds(pl.multiple_of(h * width, width), width)

    thin = height // BANDS
    per = BANDS // GROUPS

    def band_of(b):
        return pl.ds(pl.multiple_of(b * thin, thin), thin)

    def group(g):
        return pl.ds(pl.multiple_of(g * tall, tall), tall)

    def piece_rows(i):
        return group(i // parts)

    def piece_cols(i):
        return pl.ds(pl.multiple_of((i % parts) * wide, wide), wide)

    def piece_source(i):
        return pl.ds(pl.multiple_of(base + (i % parts) * wide, step), wide)

    whole_source = pl.ds(pl.multiple_of(base, step), share)

    def b_copy(u, way, row):
        return pltpu.make_async_remote_copy(
            src_ref=right.at[:, fine_source(u), :],
            dst_ref=bbuf.at[z // 2, c, :, fine_span(u), :],
            send_sem=bsend.at[way], recv_sem=brecv.at[z // 2, u],
            **other(row=row, col=y * 2 + parity))

    def b_sent(way):
        return pltpu.make_async_remote_copy(
            src_ref=right.at[:, whole_source, :], dst_ref=bbuf.at[z // 2, c],
            send_sem=bsend.at[way], recv_sem=bown.at[1], **other(**partner))

    b_local = pltpu.make_async_copy(right.at[:, whole_source, :], bbuf.at[z // 2, c], bown.at[0])
    b_partner = b_sent(2)

    def y_part(i):
        return (i == tail).astype(jnp.int32) if not isinstance(i, int) else int(i == tail)

    def y_copy(i):
        return pltpu.make_async_remote_copy(
            src_ref=left.at[:, :, source_span(i)], dst_ref=abuf.at[y, :, :, span(i)],
            send_sem=ysend.at[y_part(i)], recv_sem=yrecv.at[i], **other(**across))

    def y_piece(i):
        return pltpu.make_async_remote_copy(
            src_ref=left.at[:, piece_rows(i), piece_source(i)],
            dst_ref=abuf.at[y, :, piece_rows(i), piece_cols(i)],
            send_sem=ysend.at[y_part(i)], recv_sem=yrecv.at[i], **other(**across))

    def late(i):
        return i >= kept

    late_span = pl.ds(kept * step, EXTRA * step)
    late_source = pl.ds(pl.multiple_of(base + kept * step, step), EXTRA * step)

    def y_sent(part):
        size = (tail if part == 0 else 1) * step
        ref = abuf.at[y, :, :, pl.ds(0, size)]
        return pltpu.make_async_remote_copy(
            src_ref=ref, dst_ref=ref, send_sem=ysend.at[part], recv_sem=yrecv.at[0], **other(**across))

    def y_arrival(i):
        ref = abuf.at[1 - y, :, :, span(i)]
        return pltpu.make_async_copy(ref, ref, yrecv.at[i])

    def y_piece_arrival(i):
        ref = abuf.at[1 - y, :, piece_rows(i), piece_cols(i)]
        return pltpu.make_async_copy(ref, ref, yrecv.at[i])

    def by_piece(i, act):
        @pl.when(i % parts == 0)
        def _():
            act(piece_rows(i), fill, pl.multiple_of(base + fill, step), wide - fill)

        @pl.when(i % parts != 0)
        def _():
            start = pl.multiple_of((i % parts) * wide, wide)
            act(piece_rows(i), start, pl.multiple_of(base + start, step), wide)

    def x_own(i):
        def act(band, start, source, size):
            pltpu.make_async_remote_copy(
                src_ref=left.at[:, band, pl.ds(source, size)],
                dst_ref=xbuf.at[:, band, pl.ds(start, size)],
                send_sem=xsend, recv_sem=xrecv.at[i], **other(row=inward)).start()
        by_piece(i, act)

    def x_relay(i):
        def act(band, start, source, size):
            pltpu.make_async_remote_copy(
                src_ref=abuf.at[1 - y, :, band, pl.ds(start, size)],
                dst_ref=xbuf.at[:, band, pl.ds(start, size)],
                send_sem=xsend, recv_sem=xrecv.at[i], **other(row=inward)).start()
        by_piece(i, act)

    lent_ref = xbuf.at[:, :, pl.ds(fill, share - fill)]
    x_sent = pltpu.make_async_remote_copy(
        src_ref=lent_ref, dst_ref=lent_ref, send_sem=xsend, recv_sem=xrecv.at[0], **other(row=inward))
    e_own = pltpu.make_async_remote_copy(
        src_ref=left.at[:, :, late_source], dst_ref=ebuf,
        send_sem=esem.at[0], recv_sem=esem.at[1], **other(row=inward))
    e_relay = pltpu.make_async_remote_copy(
        src_ref=abuf.at[1 - y, :, :, late_span], dst_ref=ebuf,
        send_sem=esem.at[0], recv_sem=esem.at[1], **other(row=inward))

    yields = at_end & jnp.logical_not(lends) & (y == lent_slot)
    sends_up = (z < last) & (z != last - 1)
    sends_down = (z > 0) & (z != 1)

    fills_down = z == 1
    fills_up = z == last - 1
    fill_row = jnp.where(fills_down, 0, last)

    @pl.when(fills_down | fills_up)
    def _():
        for u in range(FILL * FINE):
            b_copy(u, 3, fill_row).start()

    @pl.when(lends_relayed)
    def _():
        for i in range(kept, CHUNKS):
            y_copy(i).start()

    def launch(i, carry):
        for k in range(FINE):
            @pl.when(sends_up)
            def _():
                b_copy(i * FINE + k, 0, z + 1).start()

            @pl.when(sends_down)
            def _():
                b_copy(i * FINE + k, 1, z - 1).start()

        @pl.when(jnp.logical_not(yields | lends_own) & jnp.logical_not(lends_relayed & late(i)))
        def _():
            y_copy(i).start()

        @pl.when(lends_own)
        def _():
            y_piece(i).start()

        return carry

    lax.fori_loop(0, CHUNKS, launch, 0)

    @pl.when(c == parity)
    def _():
        b_local.start()

    @pl.when(c != parity)
    def _():
        b_partner.start()

    @pl.when(lends_relayed)
    def _():
        e_own.start()

    @pl.when(lends_own)
    def _():
        for i in range(kept, CHUNKS):
            y_arrival(i).wait()
        e_relay.start()

        def lend(i, carry):
            x_own(i)
            return carry
        lax.fori_loop(0, CHUNKS, lend, 0)
        y_sent(0).wait_send()
        pl.semaphore_signal(turn, inc=1, **other(**partner))

    @pl.when(yields)
    def _():
        pl.semaphore_wait(turn, 1)

        def cross(i, carry):
            y_copy(i).start()
            return carry
        lax.fori_loop(0, CHUNKS, cross, 0)

    own_copy.wait()

    @pl.when(c == parity)
    def _():
        b_local.wait()
        b_sent(2).wait_recv()

    def b_arrival(s, u):
        ref = bbuf.at[s, :, :, fine_span(u), :]
        return pltpu.make_async_copy(ref, ref, brecv.at[s, u])

    def relay(s, u, part, row):
        ref = bbuf.at[s, :, :, fine_span(u), :]
        return pltpu.make_async_remote_copy(
            src_ref=ref, dst_ref=ref, send_sem=rsend.at[s, part], recv_sem=brecv.at[s, u],
            **other(row=row))

    def half_relay(s, h, row):
        ref = bbuf.at[s, h, :, late_span, :]
        return pltpu.make_async_remote_copy(
            src_ref=ref, dst_ref=ref, send_sem=rsend.at[s, 1],
            recv_sem=brecv.at[s, kept * FINE + h], **other(row=row))

    def relayed(s, part):
        start, size = ((0, kept) if part == 0 else (kept, EXTRA))
        ref = bbuf.at[s, :, :, pl.ds(start * step, size * step), :]
        return pltpu.make_async_remote_copy(
            src_ref=ref, dst_ref=ref, send_sem=rsend.at[s, part], recv_sem=brecv.at[s, 0],
            **other(row=inward))

    def present(s):
        quarter = 2 * s + c
        return jnp.logical_not((at_low & (quarter == 1)) | (at_high & (quarter == last - 1)))

    def is_own(s):
        return 2 * s + c == z

    def is_outer(s):
        outer = jnp.where(z < rows // 2, 0, last)
        return (2 * s + c == outer) & jnp.logical_not(at_end)

    def is_far(s):
        return 2 * s + c == far

    def goes_up(s):
        quarter = 2 * s + c
        return (quarter < z) & (z < last)

    def goes_down(s):
        quarter = 2 * s + c
        return (quarter > z) & (z > 0)

    def goes(s, i):
        cut = is_far(s) & ((z == 1) | (z == last - 1)) & late(i)
        return (goes_up(s) | goes_down(s)) & jnp.logical_not(cut)

    def split(value):
        high = value.astype(jnp.bfloat16)
        return high, (value - high.astype(jnp.float32)).astype(jnp.bfloat16)

    def dot(a, b):
        a_high, a_low = split(a)
        b_high, b_low = split(b)
        return jnp.dot(
            jnp.concatenate([a_high, a_high, a_low], axis=1),
            jnp.concatenate([b_high, b_low, b_high], axis=0),
            preferred_element_type=jnp.float32)

    def both(s, at):
        return (jnp.concatenate([bbuf[s, h, k, at, :] for h in range(2)], axis=1) for k in range(2))

    def accumulate(a_ref, s, at):
        a_re, a_im = a_ref[0, :, at], a_ref[1, :, at]
        b_re, b_im = both(s, at)
        acc[0] += dot(a_re, b_re)
        acc[1] += dot(a_im, b_im)
        acc[2] += dot(a_re + a_im, b_re + b_im)

    def multiply(a_ref, s, i):

        @pl.when((i % 2 == 1) & jnp.logical_not(at_end & is_far(s) & late(i)))
        def _():
            accumulate(a_ref, s, pl.ds(pl.multiple_of((i - 1) * step, 2 * step), 2 * step))

    def lent_step(i):
        def act(band, start, source, size):
            ref = xbuf.at[:, band, pl.ds(start, size)]
            pltpu.make_async_copy(ref, ref, xrecv.at[i]).wait()
            at = pl.ds(start, size)
            a_re, a_im = xbuf[0, band, at], xbuf[1, band, at]
            b_re, b_im = both(z // 2, at)
            xacc[0, band] += dot(a_re, b_re)
            xacc[1, band] += dot(a_im, b_im)
            xacc[2, band] += dot(a_re + a_im, b_re + b_im)
        by_piece(i, act)

    def combined(totals, h, g):
        first, second, third = (totals[k, group(g), half(h)] for k in range(3))
        return first - second, third - first - second

    def lend_back(h, b):
        return pltpu.make_async_remote_copy(
            src_ref=xout.at[h, :, band_of(b)], dst_ref=xin.at[:, band_of(b)],
            send_sem=csend.at[h], recv_sem=crecv.at[b], **other(row=outward, col=y * 2 + h))

    def lent_back(h):
        return pltpu.make_async_remote_copy(
            src_ref=xout.at[h], dst_ref=xin, send_sem=csend.at[h], recv_sem=crecv.at[0],
            **other(row=outward, col=y * 2 + h))

    def lent_arrival(b):
        ref = xin.at[:, band_of(b)]
        return pltpu.make_async_copy(ref, ref, crecv.at[b])

    def give(h, g):
        xout[h, 0, group(g)], xout[h, 1, group(g)] = combined(xacc, h, g)
        for k in range(per):
            lend_back(h, g * per + k).start()

    def extra_step(h):
        if h == 0:
            e_own.wait_recv()

        b_re, b_im = (bbuf[1 - z // 2, h, k, late_span, :] for k in range(2))
        b_sum = b_re + b_im
        lanes = half(h)

        for g in range(GROUPS):
            band = group(g)
            a_re, a_im = ebuf[0, band, :], ebuf[1, band, :]
            xacc[0, band, lanes] += dot(a_re, b_re)
            xacc[1, band, lanes] += dot(a_im, b_im)
            xacc[2, band, lanes] += dot(a_re + a_im, b_sum)
            if h == 1 or g < GROUPS - 1:
                give(h, g)

    def right_step(i):
        @pl.when(helps & (i == tail))
        def _():
            for k in range(LAG + 1):
                lent_step(i - LAG + k)
            give(0, GROUPS - 1)

        @pl.when(helps & is_own(y))
        def _():
            multiply(abuf.at[y], y, i)

        for n in range(2):
            s = jnp.where(z < rows // 2, 1 - n, n)

            @pl.when(present(s) & jnp.logical_not(is_own(s)) & jnp.logical_not(at_end & is_far(s) & late(i)))
            def _():
                onward = jnp.where(goes_up(s), z + 1, z - 1)
                in_halves = late(i) & helps & is_far(s)
                by_halves = late(i) & is_outer(s)

                @pl.when(jnp.logical_not(in_halves))
                def _():
                    for k in range(FINE):
                        b_arrival(s, i * FINE + k).wait()

                        @pl.when(goes(s, i) & jnp.logical_not(by_halves))
                        def _():
                            relay(s, i * FINE + k, late(i).astype(jnp.int32), onward).start()

                @pl.when(by_halves & (i == tail))
                def _():
                    for h in range(2):
                        half_relay(s, h, onward).start()

                @pl.when(in_halves)
                def _():
                    ref = bbuf.at[s, i - kept, :, late_span, :]
                    pltpu.make_async_copy(ref, ref, brecv.at[s, kept * FINE + i - kept]).wait()

        @pl.when(helps & (i == kept))
        def _():
            extra_step(0)

        @pl.when(lends & (i == 0))
        def _():
            for u in range(FILL * FINE):
                b_arrival(lent_slot, u).wait()
            accumulate(abuf.at[lent_slot], lent_slot, pl.ds(0, fill))

        @pl.when(present(y) & jnp.logical_not(helps & is_own(y)))
        def _():
            multiply(abuf.at[y], y, i)

    def left_step(i):
        @pl.when(jnp.logical_not(lends_relayed | (lends_own & late(i))))
        def _():
            y_arrival(i).wait()

        @pl.when(lends_relayed)
        def _():
            y_piece_arrival(i).wait()
            x_relay(i)

        @pl.when(present(1 - y))
        def _():
            multiply(abuf.at[1 - y], 1 - y, i)

        @pl.when(helps & (i >= LAG) & (i < tail))
        def _():
            lent_step(i - LAG)

    early = jnp.logical_not(at_end) & (c != parity)

    def work(t, carry):
        first = t < CHUNKS
        apart = jnp.where(first, t, t - CHUNKS)
        i = jnp.where(early | lends_relayed, apart, t // 2)
        is_left = ((early & jnp.logical_not(first)) | (lends_relayed & first)
                   | (jnp.logical_not(early | lends_relayed) & (t % 2 == 1)))

        @pl.when(is_left)
        def _():
            left_step(i)

        @pl.when(jnp.logical_not(is_left))
        def _():
            right_step(i)

        return carry

    lax.fori_loop(0, 2 * CHUNKS, work, 0)

    def banded(h, b):
        first, second, third = (acc[k, band_of(b), half(h)] for k in range(3))
        return first - second, third - first - second

    def to_partner(b):
        return pltpu.make_async_remote_copy(
            src_ref=pout.at[:, band_of(b)], dst_ref=pin.at[:, band_of(b)],
            send_sem=psend, recv_sem=precv.at[b], **other(**partner))

    def to_copy(b):
        return pltpu.make_async_remote_copy(
            src_ref=qout.at[:, band_of(b)], dst_ref=qin.at[:, band_of(b)],
            send_sem=qsend, recv_sem=qrecv, **other(**copy_x))

    def hand(b, carry):
        pout[0, band_of(b)], pout[1, band_of(b)] = banded(1 - c, b)
        to_partner(b).start()
        return carry

    lax.fori_loop(0, BANDS, hand, 0)

    @pl.when(helps)
    def _():
        extra_step(1)

    def gather(b, carry):
        band = band_of(b)
        mine_re, mine_im = banded(c, b)
        to_partner(b).wait_recv()
        qout[0, band] = mine_re + pin[0, band]
        qout[1, band] = mine_im + pin[1, band]

        @pl.when(at_end)
        def _():
            lent_arrival(b).wait()
            qout[:, band] += xin[:, band]

        to_copy(b).start()
        return carry

    lax.fori_loop(0, BANDS, gather, 0)

    @pl.when(sends_up)
    def _():
        b_sent(0).wait_send()

    @pl.when(sends_down)
    def _():
        b_sent(1).wait_send()

    @pl.when(c != parity)
    def _():
        b_partner.wait_send()

    @pl.when(fills_down | fills_up)
    def _():
        ref = bbuf.at[z // 2, c, :, pl.ds(0, fill), :]
        pltpu.make_async_remote_copy(
            src_ref=ref, dst_ref=ref, send_sem=bsend.at[3], recv_sem=bown.at[1],
            **other(**partner)).wait_send()

    @pl.when(jnp.logical_not(lends_own))
    def _():
        y_sent(0).wait_send()

    y_sent(1).wait_send()

    @pl.when(lends)
    def _():
        x_sent.wait_send()
        e_own.wait_send()

    for s in range(2):
        for part in range(2):
            @pl.when(present(s) & goes(s, tail * part))
            def _():
                relayed(s, part).wait_send()

    @pl.when(helps)
    def _():
        for h in range(2):
            lent_back(h).wait_send()

    whole_part = pltpu.make_async_remote_copy(
        src_ref=pout, dst_ref=pin, send_sem=psend, recv_sem=precv.at[0], **other(**partner))
    whole_part.wait_send()

    whole_copy = pltpu.make_async_remote_copy(
        src_ref=qout, dst_ref=qin, send_sem=qsend, recv_sem=qrecv, **other(**copy_x))
    whole_copy.wait()


def lent_product(left_matrix, right_matrix, layers, rows):
    height = left_matrix.shape[1]
    width = right_matrix.shape[2]
    share = left_matrix.shape[2] // layers
    f32 = jnp.float32
    dma = pltpu.SemaphoreType.DMA
    block = (2, height, width)
    own, copied = pl.pallas_call(
        functools.partial(kernel, rows),
        out_shape=[pltpu.VMEM(block, f32)] * 2,
        in_specs=[pl.BlockSpec(memory_space=pl.ANY)] * 2,
        out_specs=[pl.BlockSpec(memory_space=pltpu.VMEM)] * 2,
        scratch_shapes=[
            pltpu.VMEM((2, 2, height, share), f32),
            pltpu.VMEM((2, 2, 2, share, width), f32),
            pltpu.VMEM((2, height, share), f32),
            pltpu.VMEM((2, height, EXTRA * share // CHUNKS), f32),
            pltpu.VMEM((3, height, 2 * width), f32),
            pltpu.VMEM((3, height, 2 * width), f32),
            pltpu.VMEM((2,) + block, f32),
            pltpu.VMEM(block, f32),
            pltpu.VMEM(block, f32),
            pltpu.VMEM(block, f32),
            dma,
            dma((4,)),
            dma((2, 2)),
            dma((2, CHUNKS * FINE)),
            dma((2,)),
            dma((2,)),
            dma((CHUNKS,)),
            dma,
            dma((CHUNKS,)),
            dma((2,)),
            dma((2,)),
            dma((BANDS,)),
            dma,
            dma((BANDS,)),
            dma,
            dma,
            pltpu.SemaphoreType.REGULAR,
        ],
        compiler_params=pltpu.CompilerParams(
            collective_id=0, has_side_effects=True, vmem_limit_bytes=60 * 2**20),
    )(left_matrix, right_matrix)
    return own + copied


def gathered_product(left_matrix, right_matrix, layers):
    layer_index = lax.axis_index("layer")
    local_cols = right_matrix.shape[2]
    left_width = left_matrix.shape[2]
    right_height = right_matrix.shape[1]
    share_width = left_width // layers
    group_count = right_height // left_width
    left_own = lax.dynamic_slice_in_dim(left_matrix, layer_index * share_width, share_width, 2)
    right_view = right_matrix.reshape(2, group_count, layers, share_width, local_cols)
    right_own = lax.dynamic_slice_in_dim(right_view, layer_index, 1, 2)
    right_own = right_own.reshape(2, group_count * share_width, local_cols)
    right_whole = lax.all_gather(right_own, "row", axis=1, tiled=True)
    left_whole = lax.all_gather(left_own, "col", axis=2, tiled=True)
    dot = functools.partial(
        jnp.dot, precision=lax.Precision.HIGHEST, preferred_element_type=jnp.float32)
    first_term = dot(left_whole[0], right_whole[0])
    second_term = dot(left_whole[1], right_whole[1])
    third_term = dot(left_whole[0] + left_whole[1], right_whole[0] + right_whole[1])
    partial_product = jnp.stack([first_term - second_term, third_term - first_term - second_term])
    return lax.psum(partial_product, "layer")


def local(left_matrix, right_matrix):
    layers = lax.axis_size("layer")
    rows = lax.axis_size("row")
    cols = lax.axis_size("col")
    if layers == 2 and rows == cols == 4:
        return lent_product(left_matrix, right_matrix, layers, rows)
    return gathered_product(left_matrix, right_matrix, layers)


def solution(mesh):
    in_specs = (P(None, "row", "col"), P(None, "row", "col"))
    out_specs = P(None, "row", "col")
    return jax.shard_map(local, mesh=mesh, in_specs=in_specs, out_specs=out_specs, check_vma=False)
```
